16 devices in a mesh: dp: 2 (over z), tp: 8 (over y, x, core).
Axes of the slice: x: 2, y: 2, z: 2, core: 2. Of those that a mesh axis runs over, the one named last changes fastest.
Arguments:
- tok_hidden: bfloat16 [128, 3072], P('dp'), parts along dimension 0
- seq_lens: int32 [128], P('dp'), parts along dimension 0
- k_cache: bfloat16 [128, 512, 8, 128], P('dp', None, 'tp'), parts along dimension 0
- v_cache: bfloat16 [128, 512, 8, 128], P('dp', None, 'tp'), parts along dimension 0
- next_tok: int32 [128], P('dp'), parts along dimension 0
- g_attn: bfloat16 [3072], replicated
- w_q: bfloat16 [3072, 3072], P(None, 'tp')
- b_q: bfloat16 [3072], P('tp')
- w_k: bfloat16 [3072, 1024], P(None, 'tp')
- b_k: bfloat16 [1024], P('tp')
- w_v: bfloat16 [3072, 1024], P(None, 'tp')
- b_v: bfloat16 [1024], P('tp')
- w_o: bfloat16 [3072, 3072], P('tp')
- g_mlp: bfloat16 [3072], replicated
- w_gate: bfloat16 [3072, 8192], P(None, 'tp')
- w_up: bfloat16 [3072, 8192], P(None, 'tp')
- w_down: bfloat16 [8192, 3072], P('tp')
- g_final: bfloat16 [3072], replicated
- w_head: bfloat16 [128256, 3072], P('tp')
Outputs:
- output 1: bfloat16 [128, 3072], P('dp'), parts along dimension 0
- output 2: bfloat16 [128, 512, 8, 128], P('dp', None, 'tp'), parts along dimension 0
- output 3: bfloat16 [128, 512, 8, 128], P('dp', None, 'tp'), parts along dimension 0
- output 4: float32 [128], P('dp'), parts along dimension 0
- output 5: float32 [128], P('dp'), parts along dimension 0
There are 2 independent parts. The reference program is written for one: setup_inputs(seed, part) draws one part's arguments, and reference() takes and returns one part's arrays. A program takes and returns all parts, laid end to end along the dimension named above; an argument that names none is the same for every part.
All inputs are finite; a program needn't handle non-finite values.
Results may differ from the reference program's by a relative error of at most 0.0134478.
Values are sent between devices in bfloat16 or wider.
A program may use at most 1 GiB of HBM per device.

```python
import math
import jax
import jax.numpy as jnp
from jax import lax

BATCH = 64
LMAX = 512
D = 3072
HEADS = 24
KV_HEADS = 8
HEAD = 128
FF = 8192
VOCAB = 128256
KV_SLOTS = 8
THETA = 1000000
EPS = 1e-6
COPIES = KV_SLOTS // KV_HEADS
GROUP = HEADS // KV_SLOTS


def rms_norm(values, gain_vec):
    vals_f32 = values.astype(jnp.float32)
    inv_rms = lax.rsqrt(jnp.mean(vals_f32 * vals_f32, axis=-1, keepdims=True) + EPS)
    return (vals_f32 * inv_rms * gain_vec.astype(jnp.float32)).astype(jnp.bfloat16)


def rotary(values, positions):
    half_dim = values.shape[-1] // 2
    inv_freq = jnp.power(float(THETA), jnp.arange(half_dim, dtype=jnp.float32) * (-2.0 / values.shape[-1]))
    angles = positions.astype(jnp.float32)[:, None] * inv_freq[None, :]
    cos_part = jnp.cos(angles)[:, None, :]
    sin_part = jnp.sin(angles)[:, None, :]
    first_half = values[..., :half_dim]
    second_half = values[..., half_dim:]
    return jnp.concatenate([first_half * cos_part - second_half * sin_part, second_half * cos_part + first_half * sin_part], axis=-1)


def draw_lengths(len_key):
    exp_key, off_key, pick_key = jax.random.split(len_key, 3)
    log_max = int(math.log2(LMAX))
    exponent = jax.random.randint(exp_key, (BATCH,), 0, log_max)
    base_len = jnp.left_shift(jnp.ones((BATCH,), jnp.int32), exponent)
    offset = jax.random.randint(off_key, (BATCH,), 0, LMAX) % base_len
    longest = jax.random.randint(pick_key, (), 0, BATCH)
    return jnp.where(jnp.arange(BATCH) == longest, LMAX - 1, base_len + offset).astype(jnp.int32)


def gaussian(rand_key, arr_shape, spread):
    return jax.random.normal(rand_key, arr_shape, jnp.float32) * spread


def setup_inputs(seed: int = 0, part: int = 0) -> dict:
    shared_keys = jax.random.split(jax.random.key(seed), 16)
    part_keys = jax.random.split(jax.random.fold_in(jax.random.key(seed + 1), part), 8)
    k_scale = math.sqrt(max(math.log(LMAX / 8.0), 1.0) / 1.25)
    k_base = gaussian(part_keys[2], (BATCH, LMAX, KV_HEADS, HEAD), k_scale)
    v_base = gaussian(part_keys[3], (BATCH, LMAX, KV_HEADS, HEAD), 1.0)
    w_k = gaussian(shared_keys[3], (D, KV_HEADS, HEAD), D ** -0.5)
    b_k = gaussian(shared_keys[4], (KV_HEADS, HEAD), 0.5)
    w_v = gaussian(shared_keys[5], (D, KV_HEADS, HEAD), D ** -0.5)
    b_v = gaussian(shared_keys[6], (KV_HEADS, HEAD), 0.5)
    return {
        'tok_hidden': gaussian(part_keys[0], (BATCH, D), 1.0).astype(jnp.bfloat16),
        'seq_lens': draw_lengths(part_keys[1]),
        'k_cache': jnp.repeat(k_base, COPIES, axis=2).astype(jnp.bfloat16),
        'v_cache': jnp.repeat(v_base, COPIES, axis=2).astype(jnp.bfloat16),
        'next_tok': jax.random.randint(part_keys[4], (BATCH,), 0, VOCAB),
        'g_attn': (1.0 + gaussian(shared_keys[0], (D,), 0.2)).astype(jnp.bfloat16),
        'w_q': gaussian(shared_keys[1], (D, HEADS * HEAD), D ** -0.5).astype(jnp.bfloat16),
        'b_q': gaussian(shared_keys[2], (HEADS * HEAD,), 0.5).astype(jnp.bfloat16),
        'w_k': jnp.repeat(w_k, COPIES, axis=1).reshape(D, KV_SLOTS * HEAD).astype(jnp.bfloat16),
        'b_k': jnp.repeat(b_k, COPIES, axis=0).reshape(KV_SLOTS * HEAD).astype(jnp.bfloat16),
        'w_v': jnp.repeat(w_v, COPIES, axis=1).reshape(D, KV_SLOTS * HEAD).astype(jnp.bfloat16),
        'b_v': jnp.repeat(b_v, COPIES, axis=0).reshape(KV_SLOTS * HEAD).astype(jnp.bfloat16),
        'w_o': gaussian(shared_keys[7], (HEADS * HEAD, D), (HEADS * HEAD) ** -0.5).astype(jnp.bfloat16),
        'g_mlp': (1.0 + gaussian(shared_keys[8], (D,), 0.2)).astype(jnp.bfloat16),
        'w_gate': gaussian(shared_keys[9], (D, FF), D ** -0.5).astype(jnp.bfloat16),
        'w_up': gaussian(shared_keys[10], (D, FF), D ** -0.5).astype(jnp.bfloat16),
        'w_down': gaussian(shared_keys[11], (FF, D), FF ** -0.5).astype(jnp.bfloat16),
        'g_final': (3.0 + gaussian(shared_keys[12], (D,), 0.5)).astype(jnp.bfloat16),
        'w_head': gaussian(shared_keys[13], (VOCAB, D), D ** -0.5).astype(jnp.bfloat16),
    }


def reference(tok_hidden, seq_lens, k_cache, v_cache, next_tok, g_attn, w_q, b_q, w_k, b_k, w_v, b_v, w_o, g_mlp, w_gate, w_up, w_down, g_final, w_head):
    normed = rms_norm(tok_hidden, g_attn)
    q_proj = jnp.dot(normed, w_q, preferred_element_type=jnp.float32) + b_q.astype(jnp.float32)
    k_proj = jnp.dot(normed, w_k, preferred_element_type=jnp.float32) + b_k.astype(jnp.float32)
    v_proj = jnp.dot(normed, w_v, preferred_element_type=jnp.float32) + b_v.astype(jnp.float32)
    q_rot = rotary(q_proj.reshape(BATCH, HEADS, HEAD), seq_lens).astype(jnp.bfloat16)
    k_new = rotary(k_proj.reshape(BATCH, KV_SLOTS, HEAD), seq_lens).astype(jnp.bfloat16)
    v_new = v_proj.reshape(BATCH, KV_SLOTS, HEAD).astype(jnp.bfloat16)
    slot_ids = jnp.arange(LMAX)
    write_mask = (slot_ids[None, :] == seq_lens[:, None])[:, :, None, None]
    k_all = jnp.where(write_mask, k_new[:, None], k_cache)
    v_all = jnp.where(write_mask, v_new[:, None], v_cache)

    def one_row(row_args):
        q_row, k_row, v_row, length = row_args
        q_grp = q_row.reshape(KV_SLOTS, GROUP, HEAD).astype(jnp.float32)
        scores = jnp.einsum('kgd,lkd->kgl', q_grp, k_row.astype(jnp.float32)) * (HEAD ** -0.5)
        scores = jnp.where((slot_ids <= length)[None, None, :], scores, -jnp.inf)
        attn_probs = jax.nn.softmax(scores, axis=-1).astype(jnp.bfloat16).astype(jnp.float32)
        attn_vals = jnp.einsum('kgl,lkd->kgd', attn_probs, v_row.astype(jnp.float32))
        return attn_vals.reshape(HEADS * HEAD).astype(jnp.bfloat16)

    attn_out = lax.map(one_row, (q_rot, k_all, v_all, seq_lens))
    attn_proj = jnp.dot(attn_out, w_o, preferred_element_type=jnp.float32)
    residual = (tok_hidden.astype(jnp.float32) + attn_proj).astype(jnp.bfloat16)
    mlp_in = rms_norm(residual, g_mlp)
    gate_proj = jnp.dot(mlp_in, w_gate, preferred_element_type=jnp.float32)
    up_proj = jnp.dot(mlp_in, w_up, preferred_element_type=jnp.float32)
    hidden = (jax.nn.silu(gate_proj) * up_proj).astype(jnp.bfloat16)
    down_proj = jnp.dot(hidden, w_down, preferred_element_type=jnp.float32)
    y_out = (residual.astype(jnp.float32) + down_proj).astype(jnp.bfloat16)
    final_norm = rms_norm(y_out, g_final)
    logits = lax.dot_general(final_norm, w_head, (((1,), (1,)), ((), ())), preferred_element_type=jnp.float32)
    norm_lse = jax.nn.logsumexp(logits, axis=-1)
    vocab_ids = jnp.arange(VOCAB)
    target = jnp.sum(jnp.where(vocab_ids[None, :] == next_tok[:, None], logits, 0.0), axis=-1)
    tok_logp = target - norm_lse
    return (y_out, k_all, v_all, tok_logp, norm_lse)
```

```python
import functools

import jax
import jax.numpy as jnp
from jax import lax
from jax.experimental import pallas as pl
from jax.experimental.pallas import tpu as pltpu
from jax.sharding import PartitionSpec as P

THETA = 1000000.0
EPS = 1e-6
MESH = pl.DeviceIdType.MESH
GROUP_ROWS = 8
HEAD_ROWS = 1024
HEAD_SLOTS = 5
FLIPS = ((1, 1, 0), (1, 1, 1), (0, 1, 0), (1, 0, 0), (0, 1, 1), (1, 0, 1), (0, 0, 1))
NT = (((1,), (1,)), ((), ()))


def rms_scaled(vals_f32, gain_f32):
    inv_rms = lax.rsqrt(jnp.mean(vals_f32 * vals_f32, axis=-1, keepdims=True) + EPS)
    return (vals_f32 * inv_rms * gain_f32).astype(jnp.bfloat16)


def attention_kernel(len_ref, x_ref, g_ref, bq_ref, bk_ref, bv_ref, cos_ref, sin_ref, wq_hbm, wk_hbm, wv_hbm, kc_hbm, vc_hbm,
                     attn_ref, ko_hbm, vo_hbm,
                     wq, wk, wv, kbuf, vbuf, normed, q_scr, kn_scr, vn_scr, o_scr, w_sem, in_sem, out_sem):
    rows, cache_len, head_dim = kbuf.shape
    heads = wq.shape[1] // head_dim
    groups = rows // GROUP_ROWS
    weight_copies = [pltpu.make_async_copy(src, dst, w_sem.at[i]) for i, (src, dst) in enumerate(((wq_hbm, wq), (wk_hbm, wk), (wv_hbm, wv)))]
    for copy in weight_copies:
        copy.start()

    def loads(g):
        part = pl.ds(g * GROUP_ROWS, GROUP_ROWS)
        return (pltpu.make_async_copy(kc_hbm.at[part], kbuf.at[part], in_sem.at[0, g]),
                pltpu.make_async_copy(vc_hbm.at[part], vbuf.at[part], in_sem.at[1, g]))

    def stores(g):
        part = pl.ds(g * GROUP_ROWS, GROUP_ROWS)
        return (pltpu.make_async_copy(kbuf.at[part], ko_hbm.at[part], out_sem.at[0, g]),
                pltpu.make_async_copy(vbuf.at[part], vo_hbm.at[part], out_sem.at[1, g]))

    for g in range(groups):
        for copy in loads(g):
            copy.start()

    normed[...] = rms_scaled(x_ref[...].astype(jnp.float32), g_ref[...].astype(jnp.float32))
    q_scr[...] = jnp.zeros_like(q_scr)
    cos_part = cos_ref[...]
    sin_part = sin_ref[...]

    def rotate(vals):
        return vals * cos_part + pltpu.roll(vals, head_dim // 2, 1) * sin_part

    for copy in weight_copies:
        copy.wait()
    q_proj = jnp.dot(normed[...], wq[...], preferred_element_type=jnp.float32) + bq_ref[...].astype(jnp.float32)
    for h in range(heads):
        q_scr[pl.ds(h, rows, stride=8), :] = rotate(q_proj[:, h * head_dim:(h + 1) * head_dim])
    k_proj = jnp.dot(normed[...], wk[...], preferred_element_type=jnp.float32) + bk_ref[...].astype(jnp.float32)
    kn_scr[...] = rotate(k_proj)
    vn_scr[...] = jnp.dot(normed[...], wv[...], preferred_element_type=jnp.float32) + bv_ref[...].astype(jnp.float32)

    tile_ids = lax.broadcasted_iota(jnp.int32, (16, head_dim), 0)
    slot_ids = lax.broadcasted_iota(jnp.int32, (8, cache_len), 1)

    def patch(buf, new_ref, row, length):
        base = pl.multiple_of((length // 16) * 16, 16)
        tile = buf[row, pl.ds(base, 16), :].astype(jnp.float32)
        new = jnp.broadcast_to(new_ref[pl.ds(row, 1), :], tile.shape)
        buf[row, pl.ds(base, 16), :] = jnp.where(tile_ids == length - base, new, tile).astype(jnp.bfloat16)

    @pl.loop(0, groups)
    def group(g):
        for copy in loads(g):
            copy.wait()
        for j in range(GROUP_ROWS):
            row = g * GROUP_ROWS + j
            length = len_ref[row]
            patch(kbuf, kn_scr, row, length)
            patch(vbuf, vn_scr, row, length)
        probs = []
        for j in range(GROUP_ROWS):
            row = g * GROUP_ROWS + j
            q_row = q_scr[pl.ds(pl.multiple_of(row * 8, 8), 8), :].astype(jnp.bfloat16)
            scores = lax.dot_general(q_row, kbuf[row], NT, preferred_element_type=jnp.float32) * (head_dim ** -0.5)
            scores = jnp.where(slot_ids <= len_ref[row], scores, -jnp.inf)
            exp_scores = jnp.exp(scores - jnp.max(scores, axis=-1, keepdims=True))
            probs.append((exp_scores / jnp.sum(exp_scores, axis=-1, keepdims=True)).astype(jnp.bfloat16))
        for j in range(GROUP_ROWS):
            row = g * GROUP_ROWS + j
            o_scr[pl.ds(pl.multiple_of(row * 8, 8), 8), :] = jnp.dot(probs[j], vbuf[row], preferred_element_type=jnp.float32)
        for copy in stores(g):
            copy.start()

    for h in range(heads):
        attn_ref[:, h * head_dim:(h + 1) * head_dim] = o_scr[pl.ds(h, rows, stride=8), :].astype(jnp.bfloat16)
    for g in range(groups):
        for copy in stores(g):
            copy.wait()


def tail_kernel(attn_ref, x_ref, gm_ref, gf_ref, tok_ref, wo_hbm, wg_hbm, wu_hbm, wd_hbm, wh_hbm,
                y_ref, logp_ref, lse_ref,
                wo, wg, wu, wd, ring, send1, recv1, send2, recv2, a_full, normed, gate_act, stat_send, stat_recv,
                w_sem, ring_sem, send_sem, recv_sem):
    rows, width = x_ref.shape
    part = width // 8
    vocab = wh_hbm.shape[0]
    ff = wg.shape[1]
    chunks = pl.cdiv(vocab, HEAD_ROWS)
    me = lax.axis_index('tp')
    my_y, my_x, my_c = me // 4, (me // 2) % 2, me % 2

    def peer(flip):
        fy, fx, fc = flip
        pos_y = 1 - my_y if fy else my_y
        pos_x = 1 - my_x if fx else my_x
        pos_c = 1 - my_c if fc else my_c
        return pos_y * 4 + pos_x * 2 + pos_c

    def columns(who):
        return pl.ds(pl.multiple_of(who * part, 128), part)

    peers = [peer(flip) for flip in FLIPS]
    wo_copy = pltpu.make_async_copy(wo_hbm, wo, w_sem.at[0])
    wo_copy.start()
    barrier = pltpu.get_barrier_semaphore()
    for who in peers:
        pl.semaphore_signal(barrier, inc=1, device_id={'tp': who}, device_id_type=MESH)

    def head_copy(i):
        start = pl.multiple_of(jnp.minimum(i * HEAD_ROWS, vocab - HEAD_ROWS), 16)
        return pltpu.make_async_copy(wh_hbm.at[pl.ds(start, HEAD_ROWS)], ring.at[i % HEAD_SLOTS], ring_sem.at[i % HEAD_SLOTS])

    mlp_copies = [pltpu.make_async_copy(src, dst, w_sem.at[i + 1]) for i, (src, dst) in enumerate(((wg_hbm, wg), (wu_hbm, wu), (wd_hbm, wd)))]
    wo_copy.wait()
    for copy in mlp_copies:
        copy.start()
    for i in range(HEAD_SLOTS):
        head_copy(i).start()
    pl.semaphore_wait(barrier, len(FLIPS))

    def scatter_sum(stage, lhs, weight, send, recv, base):
        copies = []
        for k, who in enumerate(peers):
            send[k] = jnp.dot(lhs, weight[:, columns(who)], preferred_element_type=jnp.float32).astype(jnp.bfloat16)
            copy = pltpu.make_async_remote_copy(
                src_ref=send.at[k], dst_ref=recv.at[k], send_sem=send_sem.at[stage, k], recv_sem=recv_sem.at[stage, k],
                device_id={'tp': who}, device_id_type=MESH)
            copy.start()
            copies.append(copy)
        total = jnp.dot(lhs, weight[:, columns(me)], preferred_element_type=jnp.float32)
        for k in reversed(range(len(FLIPS))):
            copies[k].wait_recv()
            total = total + recv[k].astype(jnp.float32)
        return (base + total).astype(jnp.bfloat16), copies

    def gather(stage, full):
        copies = []
        for k, who in enumerate(peers):
            copy = pltpu.make_async_remote_copy(
                src_ref=full.at[:, columns(me)], dst_ref=full.at[:, columns(me)],
                send_sem=send_sem.at[stage, k], recv_sem=recv_sem.at[stage, k],
                device_id={'tp': who}, device_id_type=MESH)
            copy.start()
            copies.append(copy)
        for k, who in enumerate(peers):
            pltpu.make_async_remote_copy(
                src_ref=full.at[:, columns(who)], dst_ref=full.at[:, columns(who)],
                send_sem=send_sem.at[stage, k], recv_sem=recv_sem.at[stage, k],
                device_id={'tp': who}, device_id_type=MESH).wait_recv()
        return copies

    pending = []
    a_part, copies = scatter_sum(0, attn_ref[...], wo, send1, recv1, x_ref[:, columns(me)].astype(jnp.float32))
    pending += copies
    a_full[:, columns(me)] = a_part
    pending += gather(1, a_full)
    normed[...] = rms_scaled(a_full[...].astype(jnp.float32), gm_ref[...].astype(jnp.float32))

    mlp_copies[0].wait()
    mlp_copies[1].wait()

    @pl.loop(0, ff // 256)
    def mlp(i):
        cols = pl.ds(pl.multiple_of(i * 256, 256), 256)
        gate = jnp.dot(normed[...], wg[:, cols], preferred_element_type=jnp.float32)
        up = jnp.dot(normed[...], wu[:, cols], preferred_element_type=jnp.float32)
        gate_act[:, cols] = (jax.nn.silu(gate) * up).astype(jnp.bfloat16)

    mlp_copies[2].wait()
    y_part, copies = scatter_sum(2, gate_act[...], wd, send2, recv2, a_full[:, columns(me)].astype(jnp.float32))
    pending += copies
    y_ref[:, columns(me)] = y_part
    pending += gather(3, y_ref)
    normed[...] = rms_scaled(y_ref[...].astype(jnp.float32), gf_ref[...].astype(jnp.float32))

    lane_ids = lax.broadcasted_iota(jnp.int32, (rows, 128), 1)
    local_tok = tok_ref[...] - me * vocab

    def head_step(i, carry):
        run_max, run_sum, run_tgt = carry
        head_copy(i).wait()
        logits = lax.dot_general(normed[...], ring[i % HEAD_SLOTS], NT, preferred_element_type=jnp.float32)

        @pl.when(i + HEAD_SLOTS < chunks)
        def _():
            head_copy(i + HEAD_SLOTS).start()

        start = jnp.minimum(i * HEAD_ROWS, vocab - HEAD_ROWS)
        slabs = []
        new_max = run_max
        for s in range(HEAD_ROWS // 128):
            ids = lane_ids + (start + s * 128)
            slab = jnp.where(ids >= i * HEAD_ROWS, logits[:, s * 128:(s + 1) * 128], -jnp.inf)
            run_tgt = run_tgt + jnp.where((ids == local_tok) & (ids >= i * HEAD_ROWS), slab, 0.0)
            new_max = jnp.maximum(new_max, slab)
            slabs.append(slab)
        run_sum = run_sum * jnp.exp(run_max - new_max)
        for slab in slabs:
            run_sum = run_sum + jnp.exp(slab - new_max)
        return new_max, run_sum, run_tgt

    zeros = jnp.zeros((rows, 128), jnp.float32)
    run_max, run_sum, run_tgt = lax.fori_loop(0, chunks, head_step, (jnp.full((rows, 128), -jnp.inf, jnp.float32), zeros, zeros))
    loc_max = jnp.max(run_max, axis=-1, keepdims=True)
    loc_sum = jnp.sum(run_sum * jnp.exp(run_max - loc_max), axis=-1, keepdims=True)
    loc_tgt = jnp.sum(run_tgt, axis=-1, keepdims=True)
    packed = jnp.where(lane_ids == 0, loc_max, jnp.where(lane_ids == 1, loc_sum, loc_tgt))
    packed = jnp.concatenate([packed, jnp.zeros((128 - rows, 128), jnp.float32)], axis=0)
    own = jnp.transpose(packed)[:8]
    stat_send[...] = own
    copies = []
    for k, who in enumerate(peers):
        copy = pltpu.make_async_remote_copy(
            src_ref=stat_send, dst_ref=stat_recv.at[k], send_sem=send_sem.at[4, k], recv_sem=recv_sem.at[4, k],
            device_id={'tp': who}, device_id_type=MESH)
        copy.start()
        copies.append(copy)
    stats = [own]
    for k in reversed(range(len(FLIPS))):
        copies[k].wait_recv()
        stats.append(stat_recv[k])
    pending += copies
    glob_max = functools.reduce(jnp.maximum, [s[0:1] for s in stats])
    exp_total = functools.reduce(jnp.add, [s[1:2] * jnp.exp(s[0:1] - glob_max) for s in stats])
    lse = glob_max + jnp.log(exp_total)
    target = functools.reduce(jnp.add, [s[2:3] for s in stats])
    lse_ref[...] = lse[:, :rows]
    logp_ref[...] = (target - lse)[:, :rows]
    for copy in pending:
        copy.wait_send()


def local_step(tok_hidden, seq_lens, k_cache, v_cache, next_tok, g_attn, w_q, b_q, w_k, b_k, w_v, b_v, w_o, g_mlp, w_gate, w_up, w_down, g_final, w_head):
    rows, width = tok_hidden.shape
    cache_shape = k_cache.shape
    cache_len, head_dim = cache_shape[1], cache_shape[3]
    bf16, f32 = jnp.bfloat16, jnp.float32
    half_dim = head_dim // 2
    inv_freq = jnp.power(THETA, jnp.arange(half_dim, dtype=f32) * (-2.0 / head_dim))
    angles = seq_lens.astype(f32)[:, None] * inv_freq[None, :]
    cos_half, sin_half = jnp.cos(angles), jnp.sin(angles)
    cos_part = jnp.concatenate([cos_half, cos_half], axis=-1)
    sin_part = jnp.concatenate([-sin_half, sin_half], axis=-1)
    flat = (rows, cache_len, head_dim)
    vmem = pl.BlockSpec(memory_space=pltpu.VMEM)
    smem = pl.BlockSpec(memory_space=pltpu.SMEM)
    hbm = pl.BlockSpec(memory_space=pl.ANY)
    groups = rows // GROUP_ROWS
    attn_out, k_all, v_all = pl.pallas_call(
        attention_kernel,
        out_shape=(jax.ShapeDtypeStruct((rows, w_q.shape[1]), bf16), jax.ShapeDtypeStruct(flat, bf16), jax.ShapeDtypeStruct(flat, bf16)),
        in_specs=[smem] + [vmem] * 7 + [hbm] * 5,
        out_specs=(vmem, hbm, hbm),
        scratch_shapes=[
            pltpu.VMEM(w_q.shape, bf16), pltpu.VMEM(w_k.shape, bf16), pltpu.VMEM(w_v.shape, bf16),
            pltpu.VMEM(flat, bf16), pltpu.VMEM(flat, bf16), pltpu.VMEM((rows, width), bf16),
            pltpu.VMEM((rows * 8, head_dim), f32), pltpu.VMEM((rows, head_dim), f32), pltpu.VMEM((rows, head_dim), f32),
            pltpu.VMEM((rows * 8, head_dim), f32),
            pltpu.SemaphoreType.DMA((3,)), pltpu.SemaphoreType.DMA((2, groups)), pltpu.SemaphoreType.DMA((2, groups)),
        ],
        compiler_params=pltpu.CompilerParams(vmem_limit_bytes=40 * 1024 * 1024),
        name='attention',
    )(seq_lens, tok_hidden, g_attn[None], b_q[None], b_k[None], b_v[None], cos_part, sin_part, w_q, w_k, w_v, k_cache.reshape(flat), v_cache.reshape(flat))

    part = width // 8
    peers = len(FLIPS)
    y_out, tok_logp, norm_lse = pl.pallas_call(
        tail_kernel,
        out_shape=(jax.ShapeDtypeStruct((rows, width), bf16), jax.ShapeDtypeStruct((1, rows), f32), jax.ShapeDtypeStruct((1, rows), f32)),
        in_specs=[vmem] * 5 + [hbm] * 5,
        out_specs=(vmem, vmem, vmem),
        scratch_shapes=[
            pltpu.VMEM(w_o.shape, bf16), pltpu.VMEM(w_gate.shape, bf16), pltpu.VMEM(w_up.shape, bf16), pltpu.VMEM(w_down.shape, bf16),
            pltpu.VMEM((HEAD_SLOTS, HEAD_ROWS, width), bf16),
            pltpu.VMEM((peers, rows, part), bf16), pltpu.VMEM((peers, rows, part), bf16),
            pltpu.VMEM((peers, rows, part), bf16), pltpu.VMEM((peers, rows, part), bf16),
            pltpu.VMEM((rows, width), bf16), pltpu.VMEM((rows, width), bf16), pltpu.VMEM((rows, w_gate.shape[1]), bf16),
            pltpu.VMEM((8, 128), f32), pltpu.VMEM((peers, 8, 128), f32),
            pltpu.SemaphoreType.DMA((4,)), pltpu.SemaphoreType.DMA((HEAD_SLOTS,)),
            pltpu.SemaphoreType.DMA((5, peers)), pltpu.SemaphoreType.DMA((5, peers)),
        ],
        compiler_params=pltpu.CompilerParams(vmem_limit_bytes=62 * 1024 * 1024, collective_id=0, has_side_effects=True),
        name='tail',
    )(attn_out, tok_hidden, g_mlp[None], g_final[None], next_tok[:, None], w_o, w_gate, w_up, w_down, w_head)
    return y_out, k_all.reshape(cache_shape), v_all.reshape(cache_shape), tok_logp.reshape(rows), norm_lse.reshape(rows)


def solution(mesh):
    row_spec = P('dp', None)
    vec_spec = P('dp')
    cache_spec = P('dp', None, 'tp', None)
    col_spec = P(None, 'tp')
    part_spec = P('tp')
    whole_spec = P(None)
    in_specs = (row_spec, vec_spec, cache_spec, cache_spec, vec_spec, whole_spec, col_spec, part_spec, col_spec, part_spec, col_spec, part_spec, P('tp', None), whole_spec, col_spec, col_spec, P('tp', None), whole_spec, P('tp', None))
    out_specs = (row_spec, cache_spec, cache_spec, vec_spec, vec_spec)
    return jax.shard_map(local_step, mesh=mesh, in_specs=in_specs, out_specs=out_specs, check_vma=False)
```

```python
import functools

import jax
import jax.numpy as jnp
import numpy as np
from jax import lax
from jax.experimental import pallas as pl
from jax.experimental.pallas import tpu as pltpu
from jax.sharding import PartitionSpec as P

THETA = 1000000.0
EPS = 1e-6
MESH = pl.DeviceIdType.MESH
GROUP_ROWS = 8
HEAD_ROWS = 512
HEAD_SLOTS = 9
DIAG, ACROSS_X, ACROSS_Y = (1, 1, 0), (0, 1, 0), (1, 0, 0)
SIBLING = (0, 0, 1)
CHIPS = (DIAG, ACROSS_X, ACROSS_Y)
FLIPS = ((1, 1, 0), (1, 1, 1), (0, 1, 0), (1, 0, 0), (0, 1, 1), (1, 0, 1), (0, 0, 1))
NT = (((1,), (1,)), ((), ()))
NN = (((1,), (0,)), ((), ()))
F32, BF16 = jnp.float32, jnp.bfloat16


def rms_scaled(out, first, vals_ref, gain_ref):
    vals = vals_ref[...].astype(F32)
    rows, width = vals.shape
    inv_rms = lax.rsqrt(jnp.mean(vals * vals, axis=-1, keepdims=True) + EPS)
    gain = gain_ref[...].astype(F32)
    for i in range(width // 128):
        cols = slice(i * 128, (i + 1) * 128)
        out[first:first + rows, cols] = (vals[:, cols] * inv_rms * gain[i:i + 1, :]).astype(BF16)


def dot(lhs, rhs, dims=NN):
    return lax.dot_general(lhs, rhs, dims, preferred_element_type=F32)


def attention_kernel(len_ref, freq_ref, g_ref, bq_ref, bk_ref, bv_ref, x_hbm, wq_hbm, wk_hbm, wv_hbm, kc_hbm, vc_hbm,
                     attn_ref, ko_hbm, vo_hbm,
                     x_ref, w_all, kbuf, vbuf, normed, q_scr, kn_scr, vn_scr, o_scr, len_col, w_sem, in_sem, out_sem):
    rows, cache_len, head_dim = kbuf.shape
    q_cols = wq_hbm.shape[1]
    heads = q_cols // head_dim
    groups = rows // GROUP_ROWS
    local = pltpu.make_async_copy
    x_copy = local(x_hbm, x_ref, w_sem.at[0])
    proj_copies = [
        local(wq_hbm, w_all.at[:, 0:q_cols], w_sem.at[1]),
        local(wk_hbm, w_all.at[:, q_cols:q_cols + head_dim], w_sem.at[2]),
        local(wv_hbm, w_all.at[:, q_cols + head_dim:q_cols + 2 * head_dim], w_sem.at[3]),
    ]
    x_copy.start()
    for copy in proj_copies:
        copy.start()

    def loads(g):
        rng = pl.ds(g * GROUP_ROWS, GROUP_ROWS)
        return local(kc_hbm.at[rng], kbuf.at[rng], in_sem.at[0, g]), local(vc_hbm.at[rng], vbuf.at[rng], in_sem.at[1, g])

    def stores(g):
        rng = pl.ds(g * GROUP_ROWS, GROUP_ROWS)
        return local(kbuf.at[rng], ko_hbm.at[rng], out_sem.at[0, g]), local(vbuf.at[rng], vo_hbm.at[rng], out_sem.at[1, g])

    for g in range(groups):
        for copy in loads(g):
            copy.start()

    for r in range(rows):
        len_col[r:r + 1, :] = jnp.full((1, head_dim), len_ref[r], jnp.int32).astype(F32)
    angles = len_col[...] * freq_ref[...]
    cos_part = jnp.cos(angles)
    lane = lax.broadcasted_iota(jnp.int32, (rows, head_dim), 1)
    sin_part = jnp.where(lane < head_dim // 2, -1.0, 1.0) * jnp.sin(angles)

    def rotate(vals):
        return vals * cos_part + pltpu.roll(vals, head_dim // 2, 1) * sin_part

    q_scr[...] = jnp.zeros_like(q_scr)
    x_copy.wait()
    rms_scaled(normed, 0, x_ref, g_ref)
    for copy in proj_copies:
        copy.wait()
    proj = dot(normed[...], w_all[...])
    for h in range(heads):
        q_scr[pl.ds(h, rows, stride=8), :] = rotate(proj[:, h * head_dim:(h + 1) * head_dim] + bq_ref[h:h + 1, :].astype(F32))
    kn_scr[...] = rotate(proj[:, q_cols:q_cols + head_dim] + bk_ref[...].astype(F32))
    vn_scr[...] = proj[:, q_cols + head_dim:q_cols + 2 * head_dim] + bv_ref[...].astype(F32)

    tile_ids = lax.broadcasted_iota(jnp.int32, (16, head_dim), 0)
    slot_ids = lax.broadcasted_iota(jnp.int32, (8, cache_len), 1)

    def patch(buf, new_ref, row, length):
        base = pl.multiple_of((length // 16) * 16, 16)
        tile = buf[row, pl.ds(base, 16), :].astype(F32)
        new = jnp.broadcast_to(new_ref[pl.ds(row, 1), :], tile.shape)
        buf[row, pl.ds(base, 16), :] = jnp.where(tile_ids == length - base, new, tile).astype(BF16)

    @pl.loop(0, groups)
    def group(g):
        for copy in loads(g):
            copy.wait()
        for j in range(GROUP_ROWS):
            row = g * GROUP_ROWS + j
            length = len_ref[row]
            patch(kbuf, kn_scr, row, length)
            patch(vbuf, vn_scr, row, length)
        for copy in stores(g):
            copy.start()
        probs = []
        for j in range(GROUP_ROWS):
            row = g * GROUP_ROWS + j
            q_row = q_scr[pl.ds(pl.multiple_of(row * 8, 8), 8), :].astype(BF16)
            scores = dot(q_row, kbuf[row], NT) * (head_dim ** -0.5)
            scores = jnp.where(slot_ids <= len_ref[row], scores, -jnp.inf)
            exp_scores = jnp.exp(scores - jnp.max(scores, axis=-1, keepdims=True))
            probs.append((exp_scores / jnp.sum(exp_scores, axis=-1, keepdims=True)).astype(BF16))
        for j in range(GROUP_ROWS):
            row = g * GROUP_ROWS + j
            o_scr[pl.ds(pl.multiple_of(row * 8, 8), 8), :] = dot(probs[j], vbuf[row])

    for h in range(heads):
        attn_ref[:, h * head_dim:(h + 1) * head_dim] = o_scr[pl.ds(h, rows, stride=8), :].astype(BF16)
    for g in range(groups):
        for copy in stores(g):
            copy.wait()


def tail_kernel(tok_ref, gm_ref, gf_ref, attn_ref, x_ref, wo_hbm, wg_hbm, wu_hbm, wd_hbm, wh_hbm,
                y_ref, stat_ref,
                wo, wg, wu, wd, ring, tok_col,
                send_buf, recv1, recv2, a_full, y_full, normed, gate_act, logits_a, logits_b, run_max, run_sum, run_tgt, stat_send, stat_recv,
                w_sem, ring_sem, send_sem, recv_sem):
    rows, width = x_ref.shape
    part = width // 8
    vocab = wh_hbm.shape[0]
    half_vocab = vocab // 2
    chunks = pl.cdiv(half_vocab, HEAD_ROWS)
    ff = wg.shape[1]
    me = lax.axis_index('tp')
    plane = lax.axis_index('dp')
    my_y, my_x, my_c = me // 4, (me // 2) % 2, me % 2

    def peer(flip):
        fy, fx, fc = flip
        pos_y = 1 - my_y if fy else my_y
        pos_x = 1 - my_x if fx else my_x
        pos_c = 1 - my_c if fc else my_c
        return pos_y * 4 + pos_x * 2 + pos_c

    def columns(who):
        return pl.ds(pl.multiple_of(who * part, 128), part)

    def local(src, dst, sem):
        return pltpu.make_async_copy(src, dst, sem)

    pending = []

    def remote(src, dst, stage, slot, device):
        return pltpu.make_async_remote_copy(
            src_ref=src, dst_ref=dst, send_sem=send_sem.at[stage, slot], recv_sem=recv_sem.at[stage, slot],
            device_id=device, device_id_type=MESH)

    def push(src, dst, stage, slot, device):
        copy = remote(src, dst, stage, slot, device)
        copy.start()
        pending.append(copy)
        return copy

    wo_copy = local(wo_hbm, wo, w_sem.at[0])
    wg_copy = local(wg_hbm, wg, w_sem.at[1])
    wu_copy = local(wu_hbm, wu, w_sem.at[2])
    wd_copy = local(wd_hbm, wd, w_sem.at[3])
    wo_copy.start()
    others = [{'tp': peer(flip)} for flip in FLIPS]
    others += [{'dp': 1 - plane, 'tp': peer(flip)} for flip in FLIPS + ((0, 0, 0),)]
    barrier = pltpu.get_barrier_semaphore()
    for device in others:
        pl.semaphore_signal(barrier, inc=1, device_id=device, device_id_type=MESH)

    for r in range(rows):
        tok_col[0, r:r + 1, :] = jnp.full((1, 128), tok_ref[r], jnp.int32)

    def head_copy(i):
        start = pl.multiple_of(plane * half_vocab + jnp.minimum(i * HEAD_ROWS, half_vocab - HEAD_ROWS), 16)
        slot = i % HEAD_SLOTS
        return local(wh_hbm.at[pl.ds(start, HEAD_ROWS)], ring.at[slot], ring_sem.at[slot])

    wo_copy.wait()
    wg_copy.start()
    wu_copy.start()
    wd_copy.start()
    for i in range(HEAD_SLOTS):
        head_copy(i).start()
    pl.semaphore_wait(barrier, len(others))
    push(tok_col.at[0], tok_col.at[1], 4, 15, {'dp': 1 - plane})

    def scatter_sum(stage, lhs, weight, recv, base):
        copies = []
        for k, flip in enumerate(FLIPS):
            who = peer(flip)
            send_buf[stage // 2, k] = dot(lhs, weight[:, columns(who)]).astype(BF16)
            copies.append(push(send_buf.at[stage // 2, k], recv.at[k], stage, k, {'tp': who}))
        total = dot(lhs, weight[:, columns(me)])
        for k in reversed(range(len(FLIPS))):
            copies[k].wait_recv()
            total = total + recv[k].astype(F32)
        return (base + total).astype(BF16)

    def gather(stage, full, planes):
        sibling = {'tp': peer(SIBLING)}

        def block(p, flip):
            return full.at[p, :, columns(peer(flip))]

        def move(p, flip, slot, device):
            push(block(p, flip), block(p, flip), stage, slot, device)

        def arrive(p, flip, slot):
            remote(block(p, flip), block(p, flip), stage, slot, sibling).wait_recv()

        own = (0, 0, 0)
        if planes == 2:
            push(block(0, own), block(1, own), stage, 14, {'dp': 1 - plane})
        for i, flip in enumerate(CHIPS):
            move(0, flip=own, slot=i, device={'tp': peer(flip)})
        move(0, own, 3, sibling)
        for p in range(planes):
            if p == 1:
                arrive(1, own, 14)
                for i, flip in enumerate(CHIPS):
                    move(1, own, 7 + i, {'tp': peer(flip)})
                move(1, own, 10, sibling)
        for p in range(planes):
            for i in (1, 2, 0):
                arrive(p, CHIPS[i], 7 * p + i)
                move(p, CHIPS[i], 7 * p + 4 + i, sibling)
        for p in range(planes):
            arrive(p, SIBLING, 7 * p + 3)
            for i in (1, 2, 0):
                fy, fx, _ = CHIPS[i]
                arrive(p, (fy, fx, 1), 7 * p + 4 + i)

    a_full[0, :, columns(me)] = scatter_sum(0, attn_ref[...], wo, recv1, x_ref[:, columns(me)].astype(F32))
    gather(1, a_full, 1)
    rms_scaled(normed, 0, a_full.at[0], gm_ref)
    wg_copy.wait()
    wu_copy.wait()

    @pl.loop(0, ff // 256)
    def mlp(i):
        cols = pl.ds(pl.multiple_of(i * 256, 256), 256)
        gate = dot(normed[0:rows], wg[:, cols])
        up = dot(normed[0:rows], wu[:, cols])
        gate_act[:, cols] = (jax.nn.silu(gate) * up).astype(BF16)

    wd_copy.wait()
    y_full[0, :, columns(me)] = scatter_sum(2, gate_act[...], wd, recv2, a_full[0, :, columns(me)].astype(F32))
    gather(3, y_full, 2)
    y_ref[...] = y_full[0]
    for p in range(2):
        rms_scaled(normed, p * rows, y_full.at[p], gf_ref)
    remote(tok_col.at[0], tok_col.at[1], 4, 15, {'dp': 1 - plane}).wait_recv()
    base = me * vocab + plane * half_vocab
    run_max[...] = jnp.full_like(run_max, -jnp.inf)
    run_sum[...] = jnp.zeros_like(run_sum)
    run_tgt[...] = jnp.zeros_like(run_tgt)
    lane_ids = lax.broadcasted_iota(jnp.int32, (16, 128), 1)

    def score(i, out):
        out[...] = dot(normed[...], ring[i % HEAD_SLOTS], NT)

    def absorb(i, logits):
        first = i * HEAD_ROWS
        start = jnp.minimum(first, half_vocab - HEAD_ROWS)
        for r in range(0, 2 * rows, 16):
            blk = slice(r, r + 16)
            local_tok = tok_col[r // rows, r % rows:r % rows + 16, :] - base
            old_max = run_max[blk]
            new_max = old_max
            tgt = run_tgt[blk]
            slabs = []
            for s in range(HEAD_ROWS // 128):
                ids = lane_ids + (start + s * 128)
                raw = logits[blk, s * 128:(s + 1) * 128]
                slab = jnp.where(ids >= first, raw, -jnp.inf)
                tgt = tgt + jnp.where(ids == jnp.where(local_tok >= first, local_tok, -1), raw, 0.0)
                new_max = jnp.maximum(new_max, slab)
                slabs.append(slab)
            total = run_sum[blk] * jnp.exp(old_max - new_max)
            for slab in slabs:
                total = total + jnp.exp(slab - new_max)
            run_max[blk] = new_max
            run_sum[blk] = total
            run_tgt[blk] = tgt

    def refill(i):
        @pl.when(i + HEAD_SLOTS < chunks)
        def _():
            head_copy(i + HEAD_SLOTS).start()

    head_copy(0).wait()
    score(0, logits_a)
    refill(0)

    @pl.loop(0, (chunks - 2) // 2)
    def head(pair):
        i = pair * 2 + 1
        head_copy(i).wait()
        head_copy(i + 1).wait()
        score(i, logits_b)
        absorb(i - 1, logits_a)
        score(i + 1, logits_a)
        absorb(i, logits_b)
        refill(i)
        refill(i + 1)

    head_copy(chunks - 1).wait()
    score(chunks - 1, logits_b)
    absorb(chunks - 2, logits_a)
    absorb(chunks - 1, logits_b)

    maxes = run_max[...]
    loc_max = jnp.max(maxes, axis=-1, keepdims=True)
    loc_sum = jnp.sum(run_sum[...] * jnp.exp(maxes - loc_max), axis=-1, keepdims=True)
    loc_tgt = jnp.sum(run_tgt[...], axis=-1, keepdims=True)
    lanes = lax.broadcasted_iota(jnp.int32, (2 * rows, 128), 1)
    own = jnp.transpose(jnp.where(lanes == 0, loc_max, jnp.where(lanes == 1, loc_sum, loc_tgt)))[0:8]
    stat_send[...] = own
    copies = [push(stat_send, stat_recv.at[k], 4, k, device) for k, device in enumerate(others)]
    stats = [own]
    for k, copy in enumerate(copies):
        copy.wait_recv()
        stats.append(stat_recv[k] if k < len(FLIPS) else pltpu.roll(stat_recv[k], rows, 1))
    glob_max = functools.reduce(jnp.maximum, [s[0:1] for s in stats])
    exp_total = functools.reduce(jnp.add, [s[1:2] * jnp.exp(s[0:1] - glob_max) for s in stats])
    stat_ref[0:1, :] = functools.reduce(jnp.add, [s[2:3] for s in stats])
    stat_ref[1:2, :] = glob_max + jnp.log(exp_total)
    for copy in pending:
        copy.wait_send()


def local_step(tok_hidden, seq_lens, k_cache, v_cache, next_tok, g_attn, w_q, b_q, w_k, b_k, w_v, b_v, w_o, g_mlp, w_gate, w_up, w_down, g_final, w_head):
    rows, width = tok_hidden.shape
    cache_shape = k_cache.shape
    cache_len, head_dim = cache_shape[1], cache_shape[3]
    flat = (rows, cache_len, head_dim)
    half_freq = np.power(np.float32(THETA), np.arange(head_dim // 2, dtype=np.float32) * np.float32(-2.0 / head_dim))
    freq = jnp.asarray(np.concatenate([half_freq, half_freq])[None].astype(np.float32))
    vmem = pl.BlockSpec(memory_space=pltpu.VMEM)
    smem = pl.BlockSpec(memory_space=pltpu.SMEM)
    hbm = pl.BlockSpec(memory_space=pltpu.HBM)
    groups = rows // GROUP_ROWS
    part = width // 8
    peers = len(FLIPS)
    attn_out, k_all, v_all = pl.pallas_call(
        attention_kernel,
        out_shape=(jax.ShapeDtypeStruct((rows, w_q.shape[1]), BF16), jax.ShapeDtypeStruct(flat, BF16), jax.ShapeDtypeStruct(flat, BF16)),
        in_specs=[smem] + [vmem] * 5 + [hbm] * 6,
        out_specs=(vmem, hbm, hbm),
        scratch_shapes=[
            pltpu.VMEM((rows, width), BF16), pltpu.VMEM((width, w_q.shape[1] + 2 * head_dim), BF16),
            pltpu.VMEM(flat, BF16), pltpu.VMEM(flat, BF16), pltpu.VMEM((rows, width), BF16),
            pltpu.VMEM((rows * 8, head_dim), F32), pltpu.VMEM((rows, head_dim), F32), pltpu.VMEM((rows, head_dim), F32),
            pltpu.VMEM((rows * 8, head_dim), F32), pltpu.VMEM((rows, head_dim), F32),
            pltpu.SemaphoreType.DMA((4,)), pltpu.SemaphoreType.DMA((2, groups)), pltpu.SemaphoreType.DMA((2, groups)),
        ],
        compiler_params=pltpu.CompilerParams(vmem_limit_bytes=67043328),
        name='attention',
    )(seq_lens, freq, g_attn.reshape(-1, 128), b_q.reshape(-1, 128), b_k.reshape(-1, 128), b_v.reshape(-1, 128),
      tok_hidden, w_q, w_k, w_v, k_cache.reshape(flat), v_cache.reshape(flat))
    y_out, stats = pl.pallas_call(
        tail_kernel,
        out_shape=(jax.ShapeDtypeStruct((rows, width), BF16), jax.ShapeDtypeStruct((8, 128), F32)),
        in_specs=[smem] + [vmem] * 4 + [hbm] * 5,
        out_specs=(vmem, vmem),
        scratch_shapes=[
            pltpu.VMEM(w_o.shape, BF16), pltpu.VMEM(w_gate.shape, BF16), pltpu.VMEM(w_up.shape, BF16), pltpu.VMEM(w_down.shape, BF16),
            pltpu.VMEM((HEAD_SLOTS, HEAD_ROWS, width), BF16), pltpu.VMEM((2, rows, 128), jnp.int32),
            pltpu.VMEM((2, peers, rows, part), BF16), pltpu.VMEM((peers, rows, part), BF16), pltpu.VMEM((peers, rows, part), BF16),
            pltpu.VMEM((1, rows, width), BF16), pltpu.VMEM((2, rows, width), BF16), pltpu.VMEM((2 * rows, width), BF16), pltpu.VMEM((rows, w_gate.shape[1]), BF16),
            pltpu.VMEM((2 * rows, HEAD_ROWS), F32), pltpu.VMEM((2 * rows, HEAD_ROWS), F32),
            pltpu.VMEM((2 * rows, 128), F32), pltpu.VMEM((2 * rows, 128), F32), pltpu.VMEM((2 * rows, 128), F32),
            pltpu.VMEM((8, 128), F32), pltpu.VMEM((2 * peers + 1, 8, 128), F32),
            pltpu.SemaphoreType.DMA((4,)), pltpu.SemaphoreType.DMA((HEAD_SLOTS,)),
            pltpu.SemaphoreType.DMA((5, 16)), pltpu.SemaphoreType.DMA((5, 16)),
        ],
        compiler_params=pltpu.CompilerParams(vmem_limit_bytes=60 * 1024 * 1024, collective_id=0, has_side_effects=True),
        name='tail',
    )(next_tok, g_mlp.reshape(-1, 128), g_final.reshape(-1, 128), attn_out, tok_hidden, w_o, w_gate, w_up, w_down, w_head)
    norm_lse = stats[1, :rows]
    return y_out, k_all.reshape(cache_shape), v_all.reshape(cache_shape), stats[0, :rows] - norm_lse, norm_lse


def solution(mesh):
    row_spec = P('dp', None)
    vec_spec = P('dp')
    cache_spec = P('dp', None, 'tp', None)
    col_spec = P(None, 'tp')
    part_spec = P('tp')
    whole_spec = P(None)
    in_specs = (row_spec, vec_spec, cache_spec, cache_spec, vec_spec, whole_spec, col_spec, part_spec, col_spec, part_spec, col_spec, part_spec, P('tp', None), whole_spec, col_spec, col_spec, P('tp', None), whole_spec, P('tp', None))
    out_specs = (row_spec, cache_spec, cache_spec, vec_spec, vec_spec)
    return jax.shard_map(local_step, mesh=mesh, in_specs=in_specs, out_specs=out_specs, check_vma=False)
```

```python
import functools

import jax
import jax.numpy as jnp
import numpy as np
from jax import lax
from jax.experimental import pallas as pl
from jax.experimental.pallas import tpu as pltpu
from jax.sharding import PartitionSpec as P

THETA = 1000000.0
EPS = 1e-6
MESH = pl.DeviceIdType.MESH
GROUP_ROWS = 8
HEAD_ROWS = 512
HEAD_SLOTS = 9
EARLY_GROUPS = 2
DIAG, ACROSS_X, ACROSS_Y = (1, 1, 0), (0, 1, 0), (1, 0, 0)
SIBLING = (0, 0, 1)
CHIPS = (DIAG, ACROSS_X, ACROSS_Y)
OWN = (0, 0, 0)
FLIPS = ((1, 1, 0), (1, 1, 1), (0, 1, 0), (1, 0, 0), (0, 1, 1), (1, 0, 1), (0, 0, 1))
NT = (((1,), (1,)), ((), ()))
NN = (((1,), (0,)), ((), ()))
F32, BF16 = jnp.float32, jnp.bfloat16


def rms_scaled(out, first, vals_ref, gain_ref):
    vals = vals_ref[...].astype(F32)
    rows, width = vals.shape
    inv_rms = lax.rsqrt(jnp.mean(vals * vals, axis=-1, keepdims=True) + EPS)
    gain = gain_ref[...].astype(F32)
    for i in range(width // 128):
        cols = slice(i * 128, (i + 1) * 128)
        out[first:first + rows, cols] = (vals[:, cols] * inv_rms * gain[i:i + 1, :]).astype(BF16)


def dot(lhs, rhs, dims=NN):
    return lax.dot_general(lhs, rhs, dims, preferred_element_type=F32)


def attention_kernel(len_hbm, freq_hbm, g_hbm, bq_hbm, bk_hbm, bv_hbm, x_hbm, wq_hbm, wk_hbm, wv_hbm, kc_hbm, vc_hbm, wo_hbm,
                     part_hbm, ko_hbm, vo_hbm,
                     len_ref, freq_ref, g_ref, bq_ref, bk_ref, bv_ref, x_ref, w_all, wo, kbuf, vbuf, normed, q_scr, kn_scr, vn_scr, o_scr, len_col, part_scr,
                     w_sem, in_sem, out_sem):
    rows, cache_len, head_dim = kbuf.shape
    q_cols = wq_hbm.shape[1]
    heads = q_cols // head_dim
    groups = rows // GROUP_ROWS
    local = pltpu.make_async_copy
    small = [local(src, dst, w_sem.at[i]) for i, (src, dst) in enumerate((
        (x_hbm, x_ref), (len_hbm, len_ref), (freq_hbm, freq_ref), (g_hbm, g_ref), (bq_hbm, bq_ref), (bk_hbm, bk_ref), (bv_hbm, bv_ref)))]
    proj_copies = [
        local(wq_hbm, w_all.at[:, 0:q_cols], w_sem.at[7]),
        local(wk_hbm, w_all.at[:, q_cols:q_cols + head_dim], w_sem.at[8]),
        local(wv_hbm, w_all.at[:, q_cols + head_dim:q_cols + 2 * head_dim], w_sem.at[9]),
    ]
    wo_copy = local(wo_hbm, wo, w_sem.at[10])
    part_copy = local(part_scr, part_hbm, w_sem.at[11])
    for copy in small + proj_copies:
        copy.start()

    def loads(g):
        rng = pl.ds(g * GROUP_ROWS, GROUP_ROWS)
        return local(kc_hbm.at[rng], kbuf.at[rng], in_sem.at[0, g]), local(vc_hbm.at[rng], vbuf.at[rng], in_sem.at[1, g])

    def stores(g):
        rng = pl.ds(g * GROUP_ROWS, GROUP_ROWS)
        return local(kbuf.at[rng], ko_hbm.at[rng], out_sem.at[0, g]), local(vbuf.at[rng], vo_hbm.at[rng], out_sem.at[1, g])

    for g in range(EARLY_GROUPS):
        for copy in loads(g):
            copy.start()
    for copy in small:
        copy.wait()
    for r in range(rows):
        len_col[r:r + 1, :] = jnp.full((1, head_dim), len_ref[r], jnp.int32).astype(F32)
    angles = len_col[...] * freq_ref[...]
    cos_part = jnp.cos(angles)
    lane = lax.broadcasted_iota(jnp.int32, (rows, head_dim), 1)
    sin_part = jnp.where(lane < head_dim // 2, -1.0, 1.0) * jnp.sin(angles)

    def rotate(vals):
        return vals * cos_part + pltpu.roll(vals, head_dim // 2, 1) * sin_part

    q_scr[...] = jnp.zeros_like(q_scr)
    rms_scaled(normed, 0, x_ref, g_ref)
    for copy in proj_copies:
        copy.wait()
    for g in range(EARLY_GROUPS, groups):
        for copy in loads(g):
            copy.start()
    wo_copy.start()
    proj = dot(normed[...], w_all[...])
    for h in range(heads):
        q_scr[pl.ds(h, rows, stride=8), :] = rotate(proj[:, h * head_dim:(h + 1) * head_dim] + bq_ref[h:h + 1, :].astype(F32))
    kn_scr[...] = rotate(proj[:, q_cols:q_cols + head_dim] + bk_ref[...].astype(F32))
    vn_scr[...] = proj[:, q_cols + head_dim:q_cols + 2 * head_dim] + bv_ref[...].astype(F32)

    tile_ids = lax.broadcasted_iota(jnp.int32, (16, head_dim), 0)
    slot_ids = lax.broadcasted_iota(jnp.int32, (8, cache_len), 1)

    def patch(buf, new_ref, row, length):
        base = pl.multiple_of((length // 16) * 16, 16)
        tile = buf[row, pl.ds(base, 16), :].astype(F32)
        new = jnp.broadcast_to(new_ref[pl.ds(row, 1), :], tile.shape)
        buf[row, pl.ds(base, 16), :] = jnp.where(tile_ids == length - base, new, tile).astype(BF16)

    @pl.loop(0, groups)
    def group(g):
        for copy in loads(g):
            copy.wait()
        for j in range(GROUP_ROWS):
            row = g * GROUP_ROWS + j
            length = len_ref[row]
            patch(kbuf, kn_scr, row, length)
            patch(vbuf, vn_scr, row, length)
        for copy in stores(g):
            copy.start()
        probs = []
        for j in range(GROUP_ROWS):
            row = g * GROUP_ROWS + j
            q_row = q_scr[pl.ds(pl.multiple_of(row * 8, 8), 8), :].astype(BF16)
            scores = dot(q_row, kbuf[row], NT) * (head_dim ** -0.5)
            scores = jnp.where(slot_ids <= len_ref[row], scores, -jnp.inf)
            exp_scores = jnp.exp(scores - jnp.max(scores, axis=-1, keepdims=True))
            probs.append((exp_scores / jnp.sum(exp_scores, axis=-1, keepdims=True)).astype(BF16))
        for j in range(GROUP_ROWS):
            row = g * GROUP_ROWS + j
            o_scr[pl.ds(pl.multiple_of(row * 8, 8), 8), :] = dot(probs[j], vbuf[row])

    attn = jnp.concatenate([o_scr[pl.ds(h, rows, stride=8), :].astype(BF16) for h in range(heads)], axis=1)
    wo_copy.wait()
    part = part_scr.shape[2]
    for d in range(part_scr.shape[0]):
        part_scr[d] = dot(attn, wo[:, d * part:(d + 1) * part]).astype(BF16)
    part_copy.start()
    for g in range(groups):
        for copy in stores(g):
            copy.wait()
    part_copy.wait()


def tail_kernel(tok_hbm, gm_hbm, gf_hbm, part_hbm, x_hbm, wg_hbm, wu_hbm, wd_hbm, wh_hbm,
                y_ref, stat_ref,
                tok_ref, gm_ref, gf_ref, part_ref, x_ref, wg, wu, ring, tok_col,
                down_ref, half_recv, chip_send, chip_recv, a_full, y_full, normed, gate_act, logits_a, logits_b, run_max, run_sum, run_tgt, stat_send, stat_recv,
                w_sem, ring_sem, send_sem, recv_sem):
    rows, part = x_ref.shape
    width = part * 8
    vocab = wh_hbm.shape[0]
    half_vocab = vocab // 2
    chunks = pl.cdiv(half_vocab, HEAD_ROWS)
    ff = wg.shape[1]
    spare = HEAD_SLOTS - ff // HEAD_ROWS
    me = lax.axis_index('tp')
    plane = lax.axis_index('dp')
    my_y, my_x, my_c = me // 4, (me // 2) % 2, me % 2

    def peer(flip):
        fy, fx, fc = flip
        pos_y = 1 - my_y if fy else my_y
        pos_x = 1 - my_x if fx else my_x
        pos_c = 1 - my_c if fc else my_c
        return pos_y * 4 + pos_x * 2 + pos_c

    def columns(who):
        return pl.ds(pl.multiple_of(who * part, 128), part)

    def local(src, dst, sem):
        return pltpu.make_async_copy(src, dst, sem)

    pending = []

    def remote(src, dst, stage, slot, device):
        return pltpu.make_async_remote_copy(
            src_ref=src, dst_ref=dst, send_sem=send_sem.at[stage, slot], recv_sem=recv_sem.at[stage, slot],
            device_id=device, device_id_type=MESH)

    def push(src, dst, stage, slot, device):
        copy = remote(src, dst, stage, slot, device)
        copy.start()
        pending.append(copy)
        return copy

    small = [local(src, dst, w_sem.at[i]) for i, (src, dst) in enumerate((
        (part_hbm, part_ref), (x_hbm.at[:, columns(me)], x_ref), (tok_hbm, tok_ref), (gm_hbm, gm_ref), (gf_hbm, gf_ref)))]
    wg_copy = local(wg_hbm, wg, w_sem.at[5])
    wu_copy = local(wu_hbm, wu, w_sem.at[6])
    wd_copies = [local(wd_hbm.at[pl.ds(i * HEAD_ROWS, HEAD_ROWS)], ring.at[spare + i], ring_sem.at[spare + i]) for i in range(ff // HEAD_ROWS)]
    for copy in small:
        copy.start()
    wg_copy.start()
    wu_copy.start()
    others = [{'tp': peer(flip)} for flip in FLIPS]
    others += [{'dp': 1 - plane, 'tp': peer(flip)} for flip in FLIPS + ((0, 0, 0),)]
    barrier = pltpu.get_barrier_semaphore()
    for device in others:
        pl.semaphore_signal(barrier, inc=1, device_id=device, device_id_type=MESH)

    def head_copy(i):
        start = pl.multiple_of(plane * half_vocab + jnp.minimum(i * HEAD_ROWS, half_vocab - HEAD_ROWS), 16)
        slot = i % HEAD_SLOTS
        return local(wh_hbm.at[pl.ds(start, HEAD_ROWS)], ring.at[slot], ring_sem.at[slot])

    for copy in small:
        copy.wait()
    for r in range(rows):
        tok_col[0, r:r + 1, :] = jnp.full((1, 128), tok_ref[r], jnp.int32)
    pl.semaphore_wait(barrier, len(others))
    push(tok_col.at[0], tok_col.at[1], 4, 15, {'dp': 1 - plane})

    sibling = {'tp': peer(SIBLING)}

    def scatter_sum(stage, source, base):
        halves = []
        for i, (fy, fx, _) in enumerate(CHIPS + (OWN,)):
            source(peer((fy, fx, 1)), i, True)
            src = part_ref.at[peer((fy, fx, 1))] if stage == 0 else down_ref.at[i]
            halves.append(push(src, half_recv.at[stage // 2, i], stage, i, sibling))
        mine = [source(peer(flip), i, False) for i, flip in enumerate(CHIPS + (OWN,))]
        copies = []
        for i, flip in enumerate(CHIPS):
            halves[i].wait_recv()
            chip_send[stage // 2, i] = (mine[i] + half_recv[stage // 2, i].astype(F32)).astype(BF16)
            copies.append(push(chip_send.at[stage // 2, i], chip_recv.at[stage // 2, i], stage, 4 + i, {'tp': peer(flip)}))
        halves[3].wait_recv()
        total = mine[3] + half_recv[stage // 2, 3].astype(F32)
        for i in (1, 2, 0):
            copies[i].wait_recv()
            total = total + chip_recv[stage // 2, i].astype(F32)
        return (base + total).astype(BF16)

    def gather(stage, full, planes):
        def block(p, flip):
            return full.at[p, :, columns(peer(flip))]

        def move(p, flip, slot, device):
            push(block(p, flip), block(p, flip), stage, slot, device)

        def arrive(p, flip, slot):
            remote(block(p, flip), block(p, flip), stage, slot, sibling).wait_recv()

        own = OWN
        if planes == 2:
            push(block(0, own), block(1, own), stage, 14, {'dp': 1 - plane})
        for i, flip in enumerate(CHIPS):
            move(0, flip=own, slot=i, device={'tp': peer(flip)})
        move(0, own, 3, sibling)
        for p in range(planes):
            if p == 1:
                arrive(1, own, 14)
                for i, flip in enumerate(CHIPS):
                    move(1, own, 7 + i, {'tp': peer(flip)})
                move(1, own, 10, sibling)
        for p in range(planes):
            for i in (1, 2, 0):
                arrive(p, CHIPS[i], 7 * p + i)
                move(p, CHIPS[i], 7 * p + 4 + i, sibling)
        for p in range(planes):
            arrive(p, SIBLING, 7 * p + 3)
            for i in (1, 2, 0):
                fy, fx, _ = CHIPS[i]
                arrive(p, (fy, fx, 1), 7 * p + 4 + i)

    def attn_source(who, i, send):
        return None if send else part_ref[who].astype(F32)

    a_full[0, :, columns(me)] = scatter_sum(0, attn_source, x_ref[...].astype(F32))
    for copy in wd_copies:
        copy.start()
    gather(1, a_full, 1)
    for i in range(3):
        head_copy(i).start()
    rms_scaled(normed, 0, a_full.at[0], gm_ref)
    wg_copy.wait()
    wu_copy.wait()

    @pl.loop(0, ff // 256)
    def mlp(i):
        cols = pl.ds(pl.multiple_of(i * 256, 256), 256)
        gate = dot(normed[0:rows], wg[:, cols])
        up = dot(normed[0:rows], wu[:, cols])
        gate_act[:, cols] = (jax.nn.silu(gate) * up).astype(BF16)

    for i in range(3, spare):
        head_copy(i).start()
    for copy in wd_copies:
        copy.wait()

    def down_source(who, i, send):
        out = None
        for j in range(ff // HEAD_ROWS):
            term = dot(gate_act[:, j * HEAD_ROWS:(j + 1) * HEAD_ROWS], ring[spare + j, :, columns(who)])
            out = term if out is None else out + term
        if send:
            down_ref[i] = out.astype(BF16)
        return out

    y_full[0, :, columns(me)] = scatter_sum(2, down_source, a_full[0, :, columns(me)].astype(F32))
    for i in range(spare, HEAD_SLOTS):
        head_copy(i).start()
    gather(3, y_full, 2)
    y_ref[...] = y_full[0]
    for p in range(2):
        rms_scaled(normed, p * rows, y_full.at[p], gf_ref)
    remote(tok_col.at[0], tok_col.at[1], 4, 15, {'dp': 1 - plane}).wait_recv()
    base = me * vocab + plane * half_vocab
    run_max[...] = jnp.full_like(run_max, -jnp.inf)
    run_sum[...] = jnp.zeros_like(run_sum)
    run_tgt[...] = jnp.zeros_like(run_tgt)
    lane_ids = lax.broadcasted_iota(jnp.int32, (16, 128), 1)

    def score(i, out):
        out[...] = dot(normed[...], ring[i % HEAD_SLOTS], NT)

    def absorb(i, logits):
        first = i * HEAD_ROWS
        start = jnp.minimum(first, half_vocab - HEAD_ROWS)
        for r in range(0, 2 * rows, 16):
            blk = slice(r, r + 16)
            local_tok = tok_col[r // rows, r % rows:r % rows + 16, :] - base
            old_max = run_max[blk]
            new_max = old_max
            tgt = run_tgt[blk]
            slabs = []
            for s in range(HEAD_ROWS // 128):
                ids = lane_ids + (start + s * 128)
                raw = logits[blk, s * 128:(s + 1) * 128]
                slab = jnp.where(ids >= first, raw, -jnp.inf)
                tgt = tgt + jnp.where(ids == jnp.where(local_tok >= first, local_tok, -1), raw, 0.0)
                new_max = jnp.maximum(new_max, slab)
                slabs.append(slab)
            total = run_sum[blk] * jnp.exp(old_max - new_max)
            for slab in slabs:
                total = total + jnp.exp(slab - new_max)
            run_max[blk] = new_max
            run_sum[blk] = total
            run_tgt[blk] = tgt

    def refill(i):
        @pl.when(i + HEAD_SLOTS < chunks)
        def _():
            head_copy(i + HEAD_SLOTS).start()

    head_copy(0).wait()
    score(0, logits_a)
    refill(0)

    @pl.loop(0, (chunks - 2) // 2)
    def head(pair):
        i = pair * 2 + 1
        head_copy(i).wait()
        head_copy(i + 1).wait()
        score(i, logits_b)
        absorb(i - 1, logits_a)
        score(i + 1, logits_a)
        absorb(i, logits_b)
        refill(i)
        refill(i + 1)

    head_copy(chunks - 1).wait()
    score(chunks - 1, logits_b)
    absorb(chunks - 2, logits_a)
    absorb(chunks - 1, logits_b)

    maxes = run_max[...]
    loc_max = jnp.max(maxes, axis=-1, keepdims=True)
    loc_sum = jnp.sum(run_sum[...] * jnp.exp(maxes - loc_max), axis=-1, keepdims=True)
    loc_tgt = jnp.sum(run_tgt[...], axis=-1, keepdims=True)
    lanes = lax.broadcasted_iota(jnp.int32, (2 * rows, 128), 1)
    own = jnp.transpose(jnp.where(lanes == 0, loc_max, jnp.where(lanes == 1, loc_sum, loc_tgt)))[0:8]
    stat_send[...] = own
    copies = [push(stat_send, stat_recv.at[k], 4, k, device) for k, device in enumerate(others)]
    stats = [own]
    for k, copy in enumerate(copies):
        copy.wait_recv()
        stats.append(stat_recv[k] if k < len(FLIPS) else pltpu.roll(stat_recv[k], rows, 1))
    glob_max = functools.reduce(jnp.maximum, [s[0:1] for s in stats])
    exp_total = functools.reduce(jnp.add, [s[1:2] * jnp.exp(s[0:1] - glob_max) for s in stats])
    stat_ref[0:1, :] = functools.reduce(jnp.add, [s[2:3] for s in stats])
    stat_ref[1:2, :] = glob_max + jnp.log(exp_total)
    for copy in pending:
        copy.wait_send()


def local_step(tok_hidden, seq_lens, k_cache, v_cache, next_tok, g_attn, w_q, b_q, w_k, b_k, w_v, b_v, w_o, g_mlp, w_gate, w_up, w_down, g_final, w_head):
    rows, width = tok_hidden.shape
    cache_shape = k_cache.shape
    cache_len, head_dim = cache_shape[1], cache_shape[3]
    flat = (rows, cache_len, head_dim)
    half_freq = np.power(np.float32(THETA), np.arange(head_dim // 2, dtype=np.float32) * np.float32(-2.0 / head_dim))
    freq = jnp.asarray(np.concatenate([half_freq, half_freq])[None].astype(np.float32))
    vmem = pl.BlockSpec(memory_space=pltpu.VMEM)
    hbm = pl.BlockSpec(memory_space=pltpu.HBM)
    groups = rows // GROUP_ROWS
    part = width // 8
    peers = len(FLIPS)
    attn_part, k_all, v_all = pl.pallas_call(
        attention_kernel,
        out_shape=(jax.ShapeDtypeStruct((8, rows, part), BF16), jax.ShapeDtypeStruct(flat, BF16), jax.ShapeDtypeStruct(flat, BF16)),
        in_specs=[hbm] * 13,
        out_specs=(hbm, hbm, hbm),
        scratch_shapes=[
            pltpu.SMEM((rows,), jnp.int32), pltpu.VMEM((1, head_dim), F32), pltpu.VMEM((width // 128, 128), BF16),
            pltpu.VMEM((w_q.shape[1] // 128, 128), BF16), pltpu.VMEM((1, 128), BF16), pltpu.VMEM((1, 128), BF16),
            pltpu.VMEM((rows, width), BF16), pltpu.VMEM((width, w_q.shape[1] + 2 * head_dim), BF16), pltpu.VMEM(w_o.shape, BF16),
            pltpu.VMEM(flat, BF16), pltpu.VMEM(flat, BF16), pltpu.VMEM((rows, width), BF16),
            pltpu.VMEM((rows * 8, head_dim), F32), pltpu.VMEM((rows, head_dim), F32), pltpu.VMEM((rows, head_dim), F32),
            pltpu.VMEM((rows * 8, head_dim), F32), pltpu.VMEM((rows, head_dim), F32), pltpu.VMEM((8, rows, part), BF16),
            pltpu.SemaphoreType.DMA((12,)), pltpu.SemaphoreType.DMA((2, groups)), pltpu.SemaphoreType.DMA((2, groups)),
        ],
        compiler_params=pltpu.CompilerParams(vmem_limit_bytes=67043328),
        name='attention',
    )(seq_lens, freq, g_attn.reshape(-1, 128), b_q.reshape(-1, 128), b_k.reshape(-1, 128), b_v.reshape(-1, 128),
      tok_hidden, w_q, w_k, w_v, k_cache.reshape(flat), v_cache.reshape(flat), w_o)
    y_out, stats = pl.pallas_call(
        tail_kernel,
        out_shape=(jax.ShapeDtypeStruct((rows, width), BF16), jax.ShapeDtypeStruct((8, 128), F32)),
        in_specs=[hbm] * 9,
        out_specs=(vmem, vmem),
        scratch_shapes=[
            pltpu.SMEM((rows,), jnp.int32), pltpu.VMEM((width // 128, 128), BF16), pltpu.VMEM((width // 128, 128), BF16),
            pltpu.VMEM((8, rows, part), BF16), pltpu.VMEM((rows, part), BF16), pltpu.VMEM(w_gate.shape, BF16), pltpu.VMEM(w_up.shape, BF16),
            pltpu.VMEM((HEAD_SLOTS, HEAD_ROWS, width), BF16), pltpu.VMEM((2, rows, 128), jnp.int32),
            pltpu.VMEM((4, rows, part), BF16), pltpu.VMEM((2, 4, rows, part), BF16), pltpu.VMEM((2, 3, rows, part), BF16), pltpu.VMEM((2, 3, rows, part), BF16),
            pltpu.VMEM((1, rows, width), BF16), pltpu.VMEM((2, rows, width), BF16), pltpu.VMEM((2 * rows, width), BF16), pltpu.VMEM((rows, w_gate.shape[1]), BF16),
            pltpu.VMEM((2 * rows, HEAD_ROWS), F32), pltpu.VMEM((2 * rows, HEAD_ROWS), F32),
            pltpu.VMEM((2 * rows, 128), F32), pltpu.VMEM((2 * rows, 128), F32), pltpu.VMEM((2 * rows, 128), F32),
            pltpu.VMEM((8, 128), F32), pltpu.VMEM((2 * peers + 1, 8, 128), F32),
            pltpu.SemaphoreType.DMA((7,)), pltpu.SemaphoreType.DMA((HEAD_SLOTS,)),
            pltpu.SemaphoreType.DMA((5, 16)), pltpu.SemaphoreType.DMA((5, 16)),
        ],
        compiler_params=pltpu.CompilerParams(vmem_limit_bytes=57 * 1024 * 1024, collective_id=0, has_side_effects=True),
        name='tail',
    )(next_tok, g_mlp.reshape(-1, 128), g_final.reshape(-1, 128), attn_part, tok_hidden, w_gate, w_up, w_down, w_head)
    norm_lse = stats[1, :rows]
    return y_out, k_all.reshape(cache_shape), v_all.reshape(cache_shape), stats[0, :rows] - norm_lse, norm_lse


def solution(mesh):
    row_spec = P('dp', None)
    vec_spec = P('dp')
    cache_spec = P('dp', None, 'tp', None)
    col_spec = P(None, 'tp')
    part_spec = P('tp')
    whole_spec = P(None)
    in_specs = (row_spec, vec_spec, cache_spec, cache_spec, vec_spec, whole_spec, col_spec, part_spec, col_spec, part_spec, col_spec, part_spec, P('tp', None), whole_spec, col_spec, col_spec, P('tp', None), whole_spec, P('tp', None))
    out_specs = (row_spec, cache_spec, cache_spec, vec_spec, vec_spec)
    return jax.shard_map(local_step, mesh=mesh, in_specs=in_specs, out_specs=out_specs, check_vma=False)
```

```python
import functools

import jax
import jax.numpy as jnp
import numpy as np
from jax import lax
from jax.experimental import pallas as pl
from jax.experimental.pallas import tpu as pltpu
from jax.sharding import PartitionSpec as P

THETA = 1000000.0
EPS = 1e-6
MESH = pl.DeviceIdType.MESH
GROUP_ROWS = 8
HEAD_ROWS = 512
HEAD_SLOTS = 9
DIAG, ACROSS_X, ACROSS_Y = (1, 1, 0), (0, 1, 0), (1, 0, 0)
SIBLING = (0, 0, 1)
CHIPS = (DIAG, ACROSS_X, ACROSS_Y)
OWN = (0, 0, 0)
FLIPS = ((1, 1, 0), (1, 1, 1), (0, 1, 0), (1, 0, 0), (0, 1, 1), (1, 0, 1), (0, 0, 1))
NT = (((1,), (1,)), ((), ()))
NN = (((1,), (0,)), ((), ()))
F32, BF16 = jnp.float32, jnp.bfloat16


def rms_scaled(out, first, blocks, gain_ref):
    vals = [block.astype(F32) for block in blocks]
    rows, part = vals[0].shape
    squares = functools.reduce(jnp.add, [v * v for v in vals])
    inv_rms = lax.rsqrt(jnp.sum(squares, axis=-1, keepdims=True) / (part * len(vals)) + EPS)
    gain = gain_ref[...].astype(F32)
    for i in range(part * len(vals) // 128):
        block, lane = divmod(i * 128, part)
        out[first:first + rows, i * 128:(i + 1) * 128] = (vals[block][:, lane:lane + 128] * inv_rms * gain[i:i + 1, :]).astype(BF16)


def dot(lhs, rhs, dims=NN):
    return lax.dot_general(lhs, rhs, dims, preferred_element_type=F32)


def attention_kernel(len_hbm, tok_hbm, freq_hbm, g_hbm, gm_hbm, gf_hbm, bq_hbm, bk_hbm, bv_hbm, x_hbm, wq_hbm, wk_hbm, wv_hbm, kc_hbm, vc_hbm, wo_hbm,
                     part_hbm, ko_hbm, vo_hbm,
                     len_ref, tok_ref, freq_ref, g_ref, bq_ref, bk_ref, bv_ref, x_ref, wq, wk, wv, wo, kbuf, vbuf, normed, q_scr, kn_scr, vn_scr, o_scr, len_col, part_scr,
                     w_sem, in_sem, out_sem):
    rows, cache_len, head_dim = kbuf.shape
    q_cols = wq_hbm.shape[1]
    heads = q_cols // head_dim
    groups = rows // GROUP_ROWS
    local = pltpu.make_async_copy
    small = [local(src, dst, w_sem.at[i]) for i, (src, dst) in enumerate((
        (x_hbm, x_ref), (len_hbm, len_ref), (freq_hbm, freq_ref), (g_hbm, g_ref), (bq_hbm, bq_ref), (bk_hbm, bk_ref), (bv_hbm, bv_ref), (tok_hbm, tok_ref)))]
    proj_copies = [
        local(wq_hbm, wq, w_sem.at[8]),
        local(wk_hbm, wk, w_sem.at[9]),
        local(wv_hbm, wv, w_sem.at[10]),
    ]
    wo_copy = local(wo_hbm, wo, w_sem.at[11])
    part_copy = local(part_scr, part_hbm, w_sem.at[12])
    gain_rows = g_ref.shape[0]
    gain_copies = [local(gm_hbm, part_scr.at[8, 0:gain_rows, 0:128], w_sem.at[13]), local(gf_hbm, part_scr.at[8, 32:32 + gain_rows, 0:128], w_sem.at[14])]
    for copy in small + proj_copies:
        copy.start()

    def loads(g):
        rng = pl.ds(g * GROUP_ROWS, GROUP_ROWS)
        return local(kc_hbm.at[rng], kbuf.at[rng], in_sem.at[0, g]), local(vc_hbm.at[rng], vbuf.at[rng], in_sem.at[1, g])

    def stores(g):
        rng = pl.ds(g * GROUP_ROWS, GROUP_ROWS)
        return local(kbuf.at[rng], ko_hbm.at[rng], out_sem.at[0, g]), local(vbuf.at[rng], vo_hbm.at[rng], out_sem.at[1, g])

    for g in range(groups):
        for copy in loads(g):
            copy.start()
    for copy in small:
        copy.wait()
    for r in range(rows):
        len_col[r:r + 1, :] = jnp.full((1, head_dim), len_ref[r], jnp.int32).astype(F32)
    angles = len_col[...] * freq_ref[...]
    cos_part = jnp.cos(angles)
    lane = lax.broadcasted_iota(jnp.int32, (rows, head_dim), 1)
    sin_part = jnp.where(lane < head_dim // 2, -1.0, 1.0) * jnp.sin(angles)

    def rotate(vals):
        return vals * cos_part + pltpu.roll(vals, head_dim // 2, 1) * sin_part

    q_scr[...] = jnp.zeros_like(q_scr)
    rms_scaled(normed, 0, [x_ref[...]], g_ref)
    for copy in proj_copies:
        copy.wait()
    wo_copy.start()
    for copy in gain_copies:
        copy.start()
    q_proj = dot(normed[...], wq[...])
    k_proj = dot(normed[...], wk[...])
    v_proj = dot(normed[...], wv[...])
    for h in range(heads):
        q_scr[pl.ds(h, rows, stride=8), :] = rotate(q_proj[:, h * head_dim:(h + 1) * head_dim] + bq_ref[h:h + 1, :].astype(F32))
    kn_scr[...] = rotate(k_proj + bk_ref[...].astype(F32))
    vn_scr[...] = v_proj + bv_ref[...].astype(F32)

    tile_ids = lax.broadcasted_iota(jnp.int32, (16, head_dim), 0)
    slot_ids = lax.broadcasted_iota(jnp.int32, (8, cache_len), 1)

    def patch(buf, new_ref, row, length):
        base = pl.multiple_of((length // 16) * 16, 16)
        tile = buf[row, pl.ds(base, 16), :].astype(F32)
        new = jnp.broadcast_to(new_ref[pl.ds(row, 1), :], tile.shape)
        buf[row, pl.ds(base, 16), :] = jnp.where(tile_ids == length - base, new, tile).astype(BF16)

    @pl.loop(0, groups)
    def group(g):
        for copy in loads(g):
            copy.wait()
        for j in range(GROUP_ROWS):
            row = g * GROUP_ROWS + j
            length = len_ref[row]
            patch(kbuf, kn_scr, row, length)
            patch(vbuf, vn_scr, row, length)
        for copy in stores(g):
            copy.start()
        probs = []
        for j in range(GROUP_ROWS):
            row = g * GROUP_ROWS + j
            q_row = q_scr[pl.ds(pl.multiple_of(row * 8, 8), 8), :].astype(BF16)
            scores = dot(q_row, kbuf[row], NT) * (head_dim ** -0.5)
            scores = jnp.where(slot_ids <= len_ref[row], scores, -jnp.inf)
            exp_scores = jnp.exp(scores - jnp.max(scores, axis=-1, keepdims=True))
            probs.append((exp_scores / jnp.sum(exp_scores, axis=-1, keepdims=True)).astype(BF16))
        for j in range(GROUP_ROWS):
            row = g * GROUP_ROWS + j
            o_scr[pl.ds(pl.multiple_of(row * 8, 8), 8), :] = dot(probs[j], vbuf[row])

    attn = jnp.concatenate([o_scr[pl.ds(h, rows, stride=8), :].astype(BF16) for h in range(heads)], axis=1)
    wo_copy.wait()
    part = part_scr.shape[2]
    for d in range(8):
        part_scr[d] = dot(attn, wo[:, d * part:(d + 1) * part]).astype(BF16)
    for copy in gain_copies:
        copy.wait()
    for r in range(rows):
        len_col[r:r + 1, :] = jnp.full((1, head_dim), tok_ref[r], jnp.int32).astype(F32)
    tok = len_col[...].astype(jnp.int32)
    digits = jnp.where(lane == 0, tok // 4096, jnp.where(lane == 1, (tok // 64) % 64, tok % 64))
    part_scr[8, :, 128:256] = digits.astype(F32).astype(BF16)
    part_copy.start()
    for g in range(groups):
        for copy in stores(g):
            copy.wait()
    part_copy.wait()


def tail_kernel(part_hbm, x_hbm, wg_hbm, wu_hbm, wd_hbm, wh_hbm,
                y_ref, stat_ref,
                part_ref, x_ref, wg, wu, ring, tok_col,
                down_ref, half_recv, chip_send, chip_recv, a_full, y_full, normed, gate_act, logits_a, logits_b, run_max, run_sum, run_tgt, stat_send, stat_recv,
                w_sem, ring_sem, send_sem, recv_sem):
    rows, part = x_ref.shape
    width = part * 8
    vocab = wh_hbm.shape[0]
    half_vocab = vocab // 2
    chunks = pl.cdiv(half_vocab, HEAD_ROWS)
    ff = wg.shape[1]
    spare = HEAD_SLOTS - ff // HEAD_ROWS
    me = lax.axis_index('tp')
    plane = lax.axis_index('dp')
    my_y, my_x, my_c = me // 4, (me // 2) % 2, me % 2

    def peer(flip):
        fy, fx, fc = flip
        pos_y = 1 - my_y if fy else my_y
        pos_x = 1 - my_x if fx else my_x
        pos_c = 1 - my_c if fc else my_c
        return pos_y * 4 + pos_x * 2 + pos_c

    def columns(who):
        return pl.ds(pl.multiple_of(who * part, 128), part)

    def local(src, dst, sem):
        return pltpu.make_async_copy(src, dst, sem)

    pending = []

    def remote(src, dst, stage, slot, device):
        return pltpu.make_async_remote_copy(
            src_ref=src, dst_ref=dst, send_sem=send_sem.at[stage, slot], recv_sem=recv_sem.at[stage, slot],
            device_id=device, device_id_type=MESH)

    def push(src, dst, stage, slot, device):
        copy = remote(src, dst, stage, slot, device)
        copy.start()
        pending.append(copy)
        return copy

    small = [local(src, dst, w_sem.at[i]) for i, (src, dst) in enumerate((
        (part_hbm, part_ref), (x_hbm.at[:, columns(me)], x_ref)))]
    gain_rows = width // 128
    gm_ref, gf_ref = part_ref.at[8, 0:gain_rows, 0:128], part_ref.at[8, 32:32 + gain_rows, 0:128]
    wg_copy = local(wg_hbm, wg, w_sem.at[2])
    wu_copy = local(wu_hbm, wu, w_sem.at[3])
    wd_copies = [local(wd_hbm.at[pl.ds(i * HEAD_ROWS, HEAD_ROWS)], ring.at[spare + i], ring_sem.at[spare + i]) for i in range(ff // HEAD_ROWS)]
    for copy in small:
        copy.start()
    wg_copy.start()
    wu_copy.start()
    others = [{'tp': peer(flip)} for flip in FLIPS]
    others += [{'dp': 1 - plane, 'tp': peer(flip)} for flip in FLIPS + ((0, 0, 0),)]
    barrier = pltpu.get_barrier_semaphore()
    for device in others:
        pl.semaphore_signal(barrier, inc=1, device_id=device, device_id_type=MESH)

    def head_copy(i):
        start = pl.multiple_of(plane * half_vocab + jnp.minimum(i * HEAD_ROWS, half_vocab - HEAD_ROWS), 16)
        slot = i % HEAD_SLOTS
        return local(wh_hbm.at[pl.ds(start, HEAD_ROWS)], ring.at[slot], ring_sem.at[slot])

    for copy in small:
        copy.wait()
    digits = part_ref[8, :, 128:256].astype(F32)
    tok = digits[:, 0:1] * 4096.0 + digits[:, 1:2] * 64.0 + digits[:, 2:3]
    tok_col[0] = jnp.broadcast_to(tok, (rows, 128)).astype(jnp.int32)
    pl.semaphore_wait(barrier, len(others))
    push(tok_col.at[0], tok_col.at[1], 4, 15, {'dp': 1 - plane})

    sibling = {'tp': peer(SIBLING)}

    def scatter_sum(stage, source, base):
        halves = []
        for i, (fy, fx, _) in enumerate(CHIPS + (OWN,)):
            source(peer((fy, fx, 1)), i, True)
        for i, (fy, fx, _) in enumerate(CHIPS + (OWN,)):
            src = part_ref.at[peer((fy, fx, 1))] if stage == 0 else down_ref.at[i]
            halves.append(push(src, half_recv.at[stage // 2, i], stage, i, sibling))
        mine = [source(peer(flip), i, False) for i, flip in enumerate(CHIPS + (OWN,))]
        copies = []
        for i, flip in enumerate(CHIPS):
            halves[i].wait_recv()
            chip_send[stage // 2, i] = (mine[i] + half_recv[stage // 2, i].astype(F32)).astype(BF16)
            copies.append(push(chip_send.at[stage // 2, i], chip_recv.at[stage // 2, i], stage, 4 + i, {'tp': peer(flip)}))
        halves[3].wait_recv()
        total = mine[3] + half_recv[stage // 2, 3].astype(F32)
        for i in (1, 2, 0):
            copies[i].wait_recv()
            total = total + chip_recv[stage // 2, i].astype(F32)
        return (base + total).astype(BF16)

    def gather(stage, full, planes):
        def block(p, flip):
            return full.at[p, peer(flip)]

        def move(p, flip, slot, device):
            push(block(p, flip), block(p, flip), stage, slot, device)

        def arrive(p, flip, slot):
            remote(block(p, flip), block(p, flip), stage, slot, sibling).wait_recv()

        own = OWN
        if planes == 2:
            push(block(0, own), block(1, own), stage, 14, {'dp': 1 - plane})
        for i, flip in enumerate(CHIPS):
            move(0, flip=own, slot=i, device={'tp': peer(flip)})
        move(0, own, 3, sibling)
        for p in range(planes):
            if p == 1:
                arrive(1, own, 14)
                for i, flip in enumerate(CHIPS):
                    move(1, own, 7 + i, {'tp': peer(flip)})
                move(1, own, 10, sibling)
        for p in range(planes):
            for i in (1, 2, 0):
                arrive(p, CHIPS[i], 7 * p + i)
                move(p, CHIPS[i], 7 * p + 4 + i, sibling)
        for p in range(planes):
            arrive(p, SIBLING, 7 * p + 3)
            for i in (1, 2, 0):
                fy, fx, _ = CHIPS[i]
                arrive(p, (fy, fx, 1), 7 * p + 4 + i)

    def attn_source(who, i, send):
        return None if send else part_ref[who].astype(F32)

    a_full[0, me] = scatter_sum(0, attn_source, x_ref[...].astype(F32))
    for copy in wd_copies:
        copy.start()
    gather(1, a_full, 1)
    for i in range(3):
        head_copy(i).start()
    rms_scaled(normed, 0, [a_full[0, d] for d in range(8)], gm_ref)
    wg_copy.wait()
    wu_copy.wait()

    @pl.loop(0, ff // 256)
    def mlp(i):
        cols = pl.ds(pl.multiple_of(i * 256, 256), 256)
        gate = dot(normed[0:rows], wg[:, cols])
        up = dot(normed[0:rows], wu[:, cols])
        gate_act[:, cols] = (jax.nn.silu(gate) * up).astype(BF16)

    for i in range(3, spare):
        head_copy(i).start()
    for copy in wd_copies:
        copy.wait()

    def down_source(who, i, send):
        out = None
        for j in range(ff // HEAD_ROWS):
            term = dot(gate_act[:, j * HEAD_ROWS:(j + 1) * HEAD_ROWS], ring[spare + j, :, columns(who)])
            out = term if out is None else out + term
        if send:
            down_ref[i] = out.astype(BF16)
        return out

    y_full[0, me] = scatter_sum(2, down_source, a_full[0, me].astype(F32))
    for i in range(spare, HEAD_SLOTS):
        head_copy(i).start()
    gather(3, y_full, 2)
    for d in range(8):
        y_ref[:, d * part:(d + 1) * part] = y_full[0, d]
    for p in range(2):
        rms_scaled(normed, p * rows, [y_full[p, d] for d in range(8)], gf_ref)
    remote(tok_col.at[0], tok_col.at[1], 4, 15, {'dp': 1 - plane}).wait_recv()
    base = me * vocab + plane * half_vocab
    run_max[...] = jnp.full_like(run_max, -jnp.inf)
    run_sum[...] = jnp.zeros_like(run_sum)
    run_tgt[...] = jnp.zeros_like(run_tgt)
    lane_ids = lax.broadcasted_iota(jnp.int32, (16, 128), 1)

    def score(i, out):
        out[...] = dot(normed[...], ring[i % HEAD_SLOTS], NT)

    def absorb(i, logits):
        first = i * HEAD_ROWS
        start = jnp.minimum(first, half_vocab - HEAD_ROWS)
        for r in range(0, 2 * rows, 16):
            blk = slice(r, r + 16)
            local_tok = tok_col[r // rows, r % rows:r % rows + 16, :] - base
            old_max = run_max[blk]
            new_max = old_max
            tgt = run_tgt[blk]
            slabs = []
            for s in range(HEAD_ROWS // 128):
                ids = lane_ids + (start + s * 128)
                raw = logits[blk, s * 128:(s + 1) * 128]
                slab = jnp.where(ids >= first, raw, -jnp.inf)
                tgt = tgt + jnp.where(ids == jnp.where(local_tok >= first, local_tok, -1), raw, 0.0)
                new_max = jnp.maximum(new_max, slab)
                slabs.append(slab)
            total = run_sum[blk] * jnp.exp(old_max - new_max)
            for slab in slabs:
                total = total + jnp.exp(slab - new_max)
            run_max[blk] = new_max
            run_sum[blk] = total
            run_tgt[blk] = tgt

    def refill(i):
        @pl.when(i + HEAD_SLOTS < chunks)
        def _():
            head_copy(i + HEAD_SLOTS).start()

    head_copy(0).wait()
    score(0, logits_a)
    refill(0)

    @pl.loop(0, (chunks - 2) // 2)
    def head(pair):
        i = pair * 2 + 1
        head_copy(i).wait()
        head_copy(i + 1).wait()
        score(i, logits_b)
        absorb(i - 1, logits_a)
        score(i + 1, logits_a)
        absorb(i, logits_b)
        refill(i)
        refill(i + 1)

    head_copy(chunks - 1).wait()
    score(chunks - 1, logits_b)
    absorb(chunks - 2, logits_a)
    absorb(chunks - 1, logits_b)

    maxes = run_max[...]
    loc_max = jnp.max(maxes, axis=-1, keepdims=True)
    loc_sum = jnp.sum(run_sum[...] * jnp.exp(maxes - loc_max), axis=-1, keepdims=True)
    loc_tgt = jnp.sum(run_tgt[...], axis=-1, keepdims=True)
    lanes = lax.broadcasted_iota(jnp.int32, (2 * rows, 128), 1)
    own = jnp.transpose(jnp.where(lanes == 0, loc_max, jnp.where(lanes == 1, loc_sum, loc_tgt)))[0:8]
    stat_send[...] = own
    copies = [push(stat_send, stat_recv.at[k], 4, k, device) for k, device in enumerate(others)]
    stats = [own]
    for k, copy in enumerate(copies):
        copy.wait_recv()
        stats.append(stat_recv[k] if k < len(FLIPS) else pltpu.roll(stat_recv[k], rows, 1))
    glob_max = functools.reduce(jnp.maximum, [s[0:1] for s in stats])
    exp_total = functools.reduce(jnp.add, [s[1:2] * jnp.exp(s[0:1] - glob_max) for s in stats])
    stat_ref[0:1, :] = functools.reduce(jnp.add, [s[2:3] for s in stats])
    stat_ref[1:2, :] = glob_max + jnp.log(exp_total)
    for copy in pending:
        copy.wait_send()


def local_step(tok_hidden, seq_lens, k_cache, v_cache, next_tok, g_attn, w_q, b_q, w_k, b_k, w_v, b_v, w_o, g_mlp, w_gate, w_up, w_down, g_final, w_head):
    rows, width = tok_hidden.shape
    cache_shape = k_cache.shape
    cache_len, head_dim = cache_shape[1], cache_shape[3]
    flat = (rows, cache_len, head_dim)
    half_freq = np.power(np.float32(THETA), np.arange(head_dim // 2, dtype=np.float32) * np.float32(-2.0 / head_dim))
    freq = jnp.asarray(np.concatenate([half_freq, half_freq])[None].astype(np.float32))
    vmem = pl.BlockSpec(memory_space=pltpu.VMEM)
    hbm = pl.BlockSpec(memory_space=pltpu.HBM)
    groups = rows // GROUP_ROWS
    part = width // 8
    peers = len(FLIPS)
    attn_part, k_all, v_all = pl.pallas_call(
        attention_kernel,
        out_shape=(jax.ShapeDtypeStruct((9, rows, part), BF16), jax.ShapeDtypeStruct(flat, BF16), jax.ShapeDtypeStruct(flat, BF16)),
        in_specs=[hbm] * 16,
        out_specs=(hbm, hbm, hbm),
        scratch_shapes=[
            pltpu.SMEM((rows,), jnp.int32), pltpu.SMEM((rows,), jnp.int32), pltpu.VMEM((1, head_dim), F32), pltpu.VMEM((width // 128, 128), BF16),
            pltpu.VMEM((w_q.shape[1] // 128, 128), BF16), pltpu.VMEM((1, 128), BF16), pltpu.VMEM((1, 128), BF16),
            pltpu.VMEM((rows, width), BF16), pltpu.VMEM(w_q.shape, BF16), pltpu.VMEM(w_k.shape, BF16), pltpu.VMEM(w_v.shape, BF16), pltpu.VMEM(w_o.shape, BF16),
            pltpu.VMEM(flat, BF16), pltpu.VMEM(flat, BF16), pltpu.VMEM((rows, width), BF16),
            pltpu.VMEM((rows * 8, head_dim), F32), pltpu.VMEM((rows, head_dim), F32), pltpu.VMEM((rows, head_dim), F32),
            pltpu.VMEM((rows * 8, head_dim), F32), pltpu.VMEM((rows, head_dim), F32), pltpu.VMEM((9, rows, part), BF16),
            pltpu.SemaphoreType.DMA((15,)), pltpu.SemaphoreType.DMA((2, groups)), pltpu.SemaphoreType.DMA((2, groups)),
        ],
        compiler_params=pltpu.CompilerParams(vmem_limit_bytes=67043328),
        name='attention',
    )(seq_lens, next_tok, freq, g_attn.reshape(-1, 128), g_mlp.reshape(-1, 128), g_final.reshape(-1, 128), b_q.reshape(-1, 128), b_k.reshape(-1, 128), b_v.reshape(-1, 128),
      tok_hidden, w_q, w_k, w_v, k_cache.reshape(flat), v_cache.reshape(flat), w_o)
    y_out, stats = pl.pallas_call(
        tail_kernel,
        out_shape=(jax.ShapeDtypeStruct((rows, width), BF16), jax.ShapeDtypeStruct((8, 128), F32)),
        in_specs=[hbm] * 6,
        out_specs=(vmem, vmem),
        scratch_shapes=[
            pltpu.VMEM((9, rows, part), BF16), pltpu.VMEM((rows, part), BF16), pltpu.VMEM(w_gate.shape, BF16), pltpu.VMEM(w_up.shape, BF16),
            pltpu.VMEM((HEAD_SLOTS, HEAD_ROWS, width), BF16), pltpu.VMEM((2, rows, 128), jnp.int32),
            pltpu.VMEM((4, rows, part), BF16), pltpu.VMEM((2, 4, rows, part), BF16), pltpu.VMEM((2, 3, rows, part), BF16), pltpu.VMEM((2, 3, rows, part), BF16),
            pltpu.VMEM((1, 8, rows, part), BF16), pltpu.VMEM((2, 8, rows, part), BF16), pltpu.VMEM((2 * rows, width), BF16), pltpu.VMEM((rows, w_gate.shape[1]), BF16),
            pltpu.VMEM((2 * rows, HEAD_ROWS), F32), pltpu.VMEM((2 * rows, HEAD_ROWS), F32),
            pltpu.VMEM((2 * rows, 128), F32), pltpu.VMEM((2 * rows, 128), F32), pltpu.VMEM((2 * rows, 128), F32),
            pltpu.VMEM((8, 128), F32), pltpu.VMEM((2 * peers + 1, 8, 128), F32),
            pltpu.SemaphoreType.DMA((4,)), pltpu.SemaphoreType.DMA((HEAD_SLOTS,)),
            pltpu.SemaphoreType.DMA((5, 16)), pltpu.SemaphoreType.DMA((5, 16)),
        ],
        compiler_params=pltpu.CompilerParams(vmem_limit_bytes=54700 * 1024, collective_id=0, has_side_effects=True),
        name='tail',
    )(attn_part, tok_hidden, w_gate, w_up, w_down, w_head)
    norm_lse = stats[1, :rows]
    return y_out, k_all.reshape(cache_shape), v_all.reshape(cache_shape), stats[0, :rows] - norm_lse, norm_lse


def solution(mesh):
    row_spec = P('dp', None)
    vec_spec = P('dp')
    cache_spec = P('dp', None, 'tp', None)
    col_spec = P(None, 'tp')
    part_spec = P('tp')
    whole_spec = P(None)
    in_specs = (row_spec, vec_spec, cache_spec, cache_spec, vec_spec, whole_spec, col_spec, part_spec, col_spec, part_spec, col_spec, part_spec, P('tp', None), whole_spec, col_spec, col_spec, P('tp', None), whole_spec, P('tp', None))
    out_specs = (row_spec, cache_spec, cache_spec, vec_spec, vec_spec)
    return jax.shard_map(local_step, mesh=mesh, in_specs=in_specs, out_specs=out_specs, check_vma=False)
```
